768 devices in a mesh: sub: 96 (over z_lo, y, core), in: 8 (over x, z_hi).
Axes of the slice: x: 4, y: 8, z: 12 (z_hi: 2, z_lo: 6; z = z_hi * 6 + z_lo), core: 2. Of those that a mesh axis runs over, the one named last changes fastest.
Arguments:
- body_load: float32 [4, 64, 32, 12288], P(None, 'in', None, 'sub'), may hold values from -6 to 6
- materials: int32 [64, 32, 12288], P('in', None, 'sub'), may hold values from 0 to 7
- material_tables: float32 [8, 4, 4], replicated
- corner_index: int32 [6144], P(('sub', 'in')), may hold values from 0 to 1023
- coarse_inverse: float32 [6144, 6144], P(('sub', 'in')), as said below
Outputs:
- interior_solution: float32 [4, 64, 32, 12288], P(None, 'in', None, 'sub')
- interface_sum: float32 [96, 4, 64, 32], P('sub', None, 'in')
The draws below stay inside these ranges and needn't reach their ends.
Inputs may be any that keep to these rules, and one draw needn't show every extreme that they name: coarse_inverse is symmetric.
All inputs are finite; a program needn't handle non-finite values.
Results may differ from the reference program's by a relative error of at most 0.0003.
Values sent between devices are 32-bit elements; how exact they have to be, the bound alone decides.
A program may use at most 32 MiB of HBM per device.

```python
import jax
import jax.numpy as jnp
from jax import lax

COMP = 4
NMAT = 8
ITERS = 3
CZ = 8
PY = 32
PX = 128
KC = 8
NZ = 64
NX = 12288
COARSE = 6144
N_SUB = 96
N_IN = 8


def draw_material_tables(key, part):
    base_draw = jax.random.normal(key, (NMAT, COMP, COMP), jnp.float32)
    square = jnp.einsum('kcd,ked->kce', base_draw, base_draw)
    return 0.5 * square + 0.5 * jnp.eye(COMP, dtype=jnp.float32)[None]


def draw_coarse_inverse(key, part):
    first_key = jax.random.fold_in(key, 11)
    second_key = jax.random.fold_in(key, 23)
    base_draw = jax.random.normal(first_key, (COARSE, COARSE), jnp.float32)
    base_draw = base_draw / jnp.sqrt(jnp.float32(COARSE))
    symmetric = (base_draw + base_draw.T) * 0.5
    on_diagonal = jnp.exp(jax.random.uniform(second_key, (COARSE,), jnp.float32, jnp.log(0.5), jnp.log(2.0)))
    return symmetric + jnp.diag(on_diagonal)


def with_ends(entries, own_key, smallest, high):
    spot = [jax.random.randint(jax.random.fold_in(own_key, axis), (), 0, length) for axis, length in enumerate(entries.shape)]
    main_axis = entries.shape.index(max(entries.shape))
    neighbour = spot[:main_axis] + [(spot[main_axis] + 1) % entries.shape[main_axis]] + spot[main_axis + 1:]
    return entries.at[tuple(spot)].set(smallest).at[tuple(neighbour)].set(high)


def level_of(rng, shape, cuts, smallest, high):
    def one(position, parts):
        heights = jax.random.uniform(jax.random.fold_in(jax.random.fold_in(rng, 6), position), (parts,), jnp.float32, smallest / len(cuts), high / len(cuts))
        return jnp.repeat(jnp.exp(heights), shape[position] // parts).reshape((-1,) + (1,) * (len(shape) - position - 1))

    gain = one(*cuts[0])
    for cut in cuts[1:]:
        gain = gain * one(*cut)
    return gain


def bell_draw(key, extent, scale, reach, cuts=(), kind=jnp.bfloat16):
    result = scale * jax.random.normal(key, extent, jnp.float32)
    if cuts:
        result = result * level_of(key, extent, cuts, -0.22, 0.18)
    return jnp.clip(result, -reach, reach).astype(kind)


def setup_inputs(seed: int = 0) -> dict:
    key_list = jax.random.split(jax.random.key(seed), 6)
    body_load = bell_draw(key_list[0], (COMP, NZ, PY, NX), 1.0, 6.0, ((1, 8), (3, 96)), jnp.float32)
    materials = with_ends(jax.random.randint(key_list[1], (NZ, PY, NX), 0, NMAT), jax.random.fold_in(key_list[1], 1), 0, NMAT - 1).astype(jnp.int32)
    material_tables = draw_material_tables(jax.random.fold_in(key_list[5], 71), 0)
    corner_index = with_ends(jax.random.randint(key_list[3], (COARSE,), 0, COMP * CZ * PY), jax.random.fold_in(key_list[3], 1), 0, (COMP * CZ * PY) - 1).astype(jnp.int32)
    coarse_inverse = draw_coarse_inverse(jax.random.fold_in(key_list[5], 71), 0)
    return {"body_load": body_load, "materials": materials, "material_tables": material_tables, "corner_index": corner_index, "coarse_inverse": coarse_inverse}


def node_tables(material, tables):
    total = jnp.zeros((COMP, COMP) + material.shape, jnp.float32)
    for material_kind in range(NMAT):
        chosen = (material == material_kind).astype(jnp.float32)
        total = total + chosen[None, None] * tables[material_kind][:, :, None, None, None]
    return total


def operate(values, gains):
    padded = jnp.pad(values, ((0, 0), (1, 1), (1, 1), (1, 1)))
    beside = padded[:, 2:, 1:-1, 1:-1] + padded[:, :-2, 1:-1, 1:-1]
    beside = beside + padded[:, 1:-1, 2:, 1:-1] + padded[:, 1:-1, :-2, 1:-1]
    beside = beside + padded[:, 1:-1, 1:-1, 2:] + padded[:, 1:-1, 1:-1, :-2]
    coupled = jnp.sum(gains * values[None], axis=1)
    return 6.0 * values + coupled - beside


def conjugate(right_side, gains):
    solution = jnp.zeros_like(right_side)
    residual = right_side
    direction = right_side
    norm_now = jnp.sum(residual * residual)
    for repeat in range(ITERS):
        applied = operate(direction, gains)
        step_size = norm_now / jnp.sum(direction * applied)
        solution = solution + step_size * direction
        residual = residual - step_size * applied
        norm_next = jnp.sum(residual * residual)
        direction = residual + (norm_next / norm_now) * direction
        norm_now = norm_next
    return solution, residual


def reference(body_load, materials, material_tables, corner_index, coarse_inverse):
    loads = body_load.reshape(COMP, NZ, PY, N_SUB, PX).transpose(3, 0, 1, 2, 4)
    kinds = materials.reshape(NZ, PY, N_SUB, PX).transpose(2, 0, 1, 3)

    def solve_block(pieces):
        gains = node_tables(pieces[1], material_tables)
        return conjugate(pieces[0], gains)

    solutions, residuals = lax.map(solve_block, (loads, kinds))
    interior_solution = solutions.transpose(1, 2, 3, 0, 4).reshape(COMP, NZ, PY, NX)
    right_face = residuals[..., PX - 1]
    left_face = residuals[..., 0]
    summed = right_face + jnp.roll(left_face, -1, axis=0)
    blocks = summed.reshape(N_SUB, COMP, N_IN, CZ, PY).transpose(0, 2, 1, 3, 4)
    blocks = blocks.reshape(N_SUB * N_IN, COMP * CZ * PY)
    corner_ids = corner_index.reshape(N_SUB * N_IN, KC).astype(jnp.int32)
    coarse_residual = jnp.take_along_axis(blocks, corner_ids, axis=1).reshape(COARSE)
    coarse_solution = jnp.dot(coarse_inverse, coarse_residual, precision=lax.Precision.HIGHEST)
    row_ids = jnp.arange(N_SUB * N_IN, dtype=jnp.int32)[:, None]
    blocks = blocks.at[row_ids, corner_ids].add(coarse_solution.reshape(N_SUB * N_IN, KC))
    interface_sum = blocks.reshape(N_SUB, N_IN, COMP, CZ, PY).transpose(0, 2, 1, 3, 4).reshape(N_SUB, COMP, NZ, PY)
    return interior_solution, interface_sum
```

```python
import jax
import jax.numpy as jnp
from jax import lax
from jax.experimental import pallas as pl
from jax.experimental.pallas import tpu as pltpu
from jax.sharding import PartitionSpec as P

MESH = pl.DeviceIdType.MESH
COMP, NMAT, ITERS = 4, 8, 3
CZ, PY, PX, KC = 8, 32, 128, 8
N_SUB, N_IN = 96, 8
H = ITERS
EXT = CZ + 2 * H
NY, NZL = 8, 6
CHIPS = N_SUB // 2
PAIRS = [(0, 0), (0, 1), (0, 2), (0, 3), (1, 1), (1, 2), (1, 3), (2, 2), (2, 3)]
ZSTEPS = (1, 2, 3, 10, 11)


def remote(src, dst, send, recv, device):
    return pltpu.make_async_remote_copy(
        src_ref=src, dst_ref=dst, send_sem=send, recv_sem=recv, device_id=device, device_id_type=MESH
    )


def kernel(
    b_hbm, m_hbm, tab, ci_hbm, cinv_hbm,
    sol_hbm, face_hbm,
    v0, v1, v2, v3, mat, gains, cinv, sol, rows, send_row, ex, ag, left_out, left_in, face,
    ci_vec, ci_left_vec, ci_own, ci_left, local_sem, send_sem, recv_sem,
):
    sub, inn = lax.axis_index("sub"), lax.axis_index("in")
    core, y, zl = sub % 2, (sub // 2) % NY, sub // (2 * NY)
    x, z = inn // 2, (inn % 2) * NZL + zl

    def device(core_, y_, z_):
        return {"sub": ((z_ % NZL) * NY + y_) * 2 + core_, "in": x * 2 + z_ // NZL}

    def in_peer(k):
        return {"sub": sub, "in": (inn + k) % N_IN}

    def z_peer(d, other):
        return device((core + other) % 2, y, (z + d) % (2 * NZL))

    def y_peer(k):
        return device(core, (y + k) % NY, z)

    sub_next = {"sub": (sub + 1) % N_SUB, "in": inn}
    sub_prev = {"sub": (sub + N_SUB - 1) % N_SUB, "in": inn}

    load_b = pltpu.make_async_copy(b_hbm, v0.at[:, pl.ds(H, CZ)], local_sem.at[0])
    load_m = pltpu.make_async_copy(m_hbm, mat.at[pl.ds(H, CZ)], local_sem.at[1])
    load_c = pltpu.make_async_copy(ci_hbm, ci_vec, local_sem.at[2])
    load_inv = pltpu.make_async_copy(cinv_hbm, cinv, local_sem.at[3])
    load_own = pltpu.make_async_copy(ci_hbm, ci_own, local_sem.at[4])
    load_b.start()
    load_m.start()
    load_c.start()
    load_own.start()
    load_inv.start()

    barrier = pltpu.get_barrier_semaphore()
    greet = [in_peer(k) for k in range(1, N_IN)]
    greet += [z_peer(d, o) for d in (0, 1, 2, 3, 9, 10, 11) for o in (0, 1) if d or o]
    greet += [y_peer(k) for k in range(1, NY)]
    greet += [sub_next, sub_prev]
    for peer in greet:
        pl.semaphore_signal(barrier, inc=1, device_id=peer, device_id_type=MESH)

    low, high = None, None
    for k in range(NMAT):
        for c in range(COMP):
            centre = tab[k, c, c]
            radius = jnp.float32(6.0)
            for d in range(COMP):
                if d != c:
                    radius = radius + jnp.maximum(tab[k, c, d], -tab[k, c, d])
            lo, hi = centre - radius, centre + radius
            low = lo if low is None else jnp.minimum(low, lo)
            high = hi if high is None else jnp.maximum(high, hi)
    sigma = 6.0 + 0.5 * (low + high)
    width = 0.5 * (high - low)
    inv_row = 1.0 / jnp.full((1, PX), width, jnp.float32)
    shift = 6.0 - sigma

    load_b.wait()
    load_m.wait()
    load_c.wait()
    load_own.wait()
    pl.semaphore_wait(barrier, len(greet))

    up, down = in_peer(1), in_peer(N_IN - 1)
    halos = [
        remote(v0.at[:, pl.ds(CZ, H)], v0.at[:, pl.ds(0, H)], send_sem.at[0], recv_sem.at[0], up),
        remote(v0.at[:, pl.ds(H, H)], v0.at[:, pl.ds(H + CZ, H)], send_sem.at[1], recv_sem.at[1], down),
        remote(mat.at[pl.ds(CZ + 1, 2)], mat.at[pl.ds(1, 2)], send_sem.at[2], recv_sem.at[2], up),
        remote(mat.at[pl.ds(H, 2)], mat.at[pl.ds(H + CZ, 2)], send_sem.at[3], recv_sem.at[3], down),
        remote(ci_vec, ci_left_vec, send_sem.at[4], recv_sem.at[4], sub_next),
    ]
    for copy in halos:
        copy.start()

    lane = lax.broadcasted_iota(jnp.int32, (PY, PX), 1)
    row = lax.broadcasted_iota(jnp.int32, (PY, PX), 0)

    def tables_of(layer):
        ids = mat[layer]
        top, mid, bottom = ids >= 4, (ids & 2) != 0, (ids & 1) != 0
        for c in range(COMP):
            for d in range(COMP):
                pairs = [jnp.where(bottom, tab[2 * k + 1, c, d], tab[2 * k, c, d]) for k in range(4)]
                value = jnp.where(top, jnp.where(mid, pairs[3], pairs[2]), jnp.where(mid, pairs[1], pairs[0]))
                gains[c * COMP + d, layer] = value + shift if c == d else value

    def apply_at(src, layer, scale):
        centre = [src[c, layer] for c in range(COMP)]
        result = []
        for c in range(COMP):
            v = centre[c]
            beside = src[c, layer - 1] + src[c, layer + 1]
            beside = beside + jnp.where(row == 0, 0.0, pltpu.roll(v, 1, 0))
            beside = beside + jnp.where(row == PY - 1, 0.0, pltpu.roll(v, PY - 1, 0))
            beside = beside + jnp.where(lane == 0, 0.0, pltpu.roll(v, 1, 1))
            beside = beside + jnp.where(lane == PX - 1, 0.0, pltpu.roll(v, PX - 1, 1))
            coupled = gains[c * COMP, layer] * centre[0]
            for d in range(1, COMP):
                coupled = coupled + gains[c * COMP + d, layer] * centre[d]
            result.append((coupled - beside) * scale)
        return centre, result

    def layers(lo, hi, body):
        @pl.loop(lo, hi)
        def _(layer):
            body(layer)

    def scale_at(layer):
        at = inn * CZ - H + layer
        keep = jnp.where((at >= 0) & (at < N_IN * CZ), jnp.float32(1.0), jnp.float32(0.0))
        return inv_row * keep

    def advance(src, dst):
        def body(layer):
            _, result = apply_at(src, layer, scale_at(layer))
            for c in range(COMP):
                dst[c, layer] = result[c]

        return body

    first, second = advance(v0, v1), advance(v1, v2)

    def third(layer, sums):
        a2, a3 = apply_at(v2, layer, inv_row)
        a0 = [v0[c, layer] for c in range(COMP)]
        a1 = [v1[c, layer] for c in range(COMP)]
        basis = (a0, a1, a2, a3)
        for c in range(COMP):
            v3[c, layer - H] = a3[c]
        out = []
        for (i, j), total in zip(PAIRS, sums):
            part = basis[i][0] * basis[j][0]
            for c in range(1, COMP):
                part = part + basis[i][c] * basis[j][c]
            out.append(total + ((part[0:8] + part[8:16]) + (part[16:24] + part[24:32])))
        return tuple(out)

    layers(H, H + CZ, tables_of)
    layers(H + 1, H + CZ - 1, first)
    layers(H + 2, H + CZ - 2, second)
    sums = tuple(jnp.zeros((8, PX), jnp.float32) for _ in PAIRS)
    sums = lax.fori_loop(H + 3, H + CZ - 3, third, sums)

    for copy in halos:
        copy.wait()
    load_left = pltpu.make_async_copy(ci_left_vec, ci_left, local_sem.at[5])
    load_left.start()

    @pl.when(inn == 0)
    def _():
        for c in range(COMP):
            v0[c, H - 1] = jnp.zeros((PY, PX), jnp.float32)

    @pl.when(inn == N_IN - 1)
    def _():
        for c in range(COMP):
            v0[c, H + CZ] = jnp.zeros((PY, PX), jnp.float32)

    layers(1, H, tables_of)
    layers(H + CZ, EXT - 1, tables_of)
    layers(1, H + 1, first)
    layers(H + CZ - 1, EXT - 1, first)
    layers(2, H + 2, second)
    layers(H + CZ - 2, EXT - 2, second)
    sums = lax.fori_loop(H, H + 3, third, sums)
    sums = lax.fori_loop(H + CZ - 3, H + CZ, third, sums)
    load_left.wait()

    for j in range(KC):
        for side, ids in ((0, ci_own), (1, ci_left)):
            spot = ids[0, j]
            c, layer, at = spot // (CZ * PY), (spot // PY) % CZ, spot % PY
            place = side * KC + j
            rows[pl.ds(place, 1), :] = v0[c, layer + H, pl.ds(at, 1), :]
            rows[pl.ds(16 + place, 1), :] = v1[c, layer + H, pl.ds(at, 1), :]
            rows[pl.ds(32 + place, 1), :] = v2[c, layer + H, pl.ds(at, 1), :]
            rows[pl.ds(48 + place, 1), :] = v3[c, layer, pl.ds(at, 1), :]
    rows[pl.ds(64, 64), :] = jnp.zeros((64, PX), jnp.float32)
    turned = jnp.transpose(rows[...])
    lane1 = lax.broadcasted_iota(jnp.int32, (1, PX), 1)
    own_row = jnp.where((lane1 // KC) % 2 == 0, turned[PX - 1 : PX, :], turned[0:1, :])
    own_row = jnp.where(lane1 < 64, own_row, 0.0)
    for n, total in enumerate(sums):
        whole = jnp.sum(jnp.sum(total, axis=0, keepdims=True), axis=1, keepdims=True)
        own_row = jnp.where(lane1 == 64 + n, whole, own_row)
    send_row[...] = own_row
    ex[pl.ds(inn, 1), :] = own_row
    gram_copies = []
    for k in range(1, N_IN):
        copy = remote(send_row, ex.at[pl.ds(inn, 1)], send_sem.at[4 + k], recv_sem.at[4 + k], in_peer(k))
        copy.start()
        gram_copies.append(copy)
    for copy in gram_copies:
        copy.wait()

    everyone = ex[...]
    total = jnp.sum(everyone, axis=0, keepdims=True)
    gram = {}
    for n, (i, j) in enumerate(PAIRS):
        value = jnp.sum(jnp.where(lane1 == 64 + n, total, 0.0), axis=1, keepdims=True)
        gram[i, j] = gram[j, i] = value

    def form(p, q, offset):
        value = None
        for i, a in enumerate(p):
            for j, b in enumerate(q):
                term = a * b * gram[i, j + offset]
                value = term if value is None else value + term
        return value

    res = [jnp.ones((1, 1), jnp.float32)]
    direction, previous = list(res), []
    rr = form(res, res, 0)
    dd, beta = rr, None
    answer = [jnp.zeros((1, 1), jnp.float32) for _ in range(ITERS)]
    for step in range(ITERS):
        delta = width * form(direction, direction, 1)
        if step:
            delta = delta + sigma * (beta * beta * dd_before)
        inverse = 1.0 / (sigma * rr + delta)
        alpha = rr * inverse
        for j, value in enumerate(direction):
            answer[j] = answer[j] + alpha * value
        moved = []
        for j in range(step + 2):
            value = None
            if j <= step:
                value = res[j] * delta
                if j < len(previous):
                    value = value - sigma * rr * (beta * previous[j])
                value = value * inverse
            if j:
                part = (alpha * width) * direction[j - 1]
                value = -part if value is None else value - part
            moved.append(value)
        if step + 1 < ITERS:
            new = form(moved, moved, 0)
            beta = new / rr
            previous = direction
            direction = [
                value + beta * direction[j] if j <= step else value for j, value in enumerate(moved)
            ]
            dd_before = dd
            dd = new + beta * beta * dd
            rr = new
        res = moved

    factors = jnp.zeros((1, PX), jnp.float32)
    for k in range(ITERS + 1):
        factors = jnp.where(lane1 // 16 == k, res[k], factors)
    mixed = everyone * factors
    mixed = (mixed + pltpu.roll(mixed, PX - 16, 1)) + (pltpu.roll(mixed, PX - 32, 1) + pltpu.roll(mixed, PX - 48, 1))
    unit = jnp.zeros((1, PX), jnp.float32)
    for i in range(N_IN):
        piece = mixed[i : i + 1, :]
        piece = jnp.where(lane1 < 8, piece, 0.0) + pltpu.roll(jnp.where((lane1 >= 8) & (lane1 < 16), piece, 0.0), 56, 1)
        unit = unit + (pltpu.roll(piece, KC * i, 1) if i else piece)

    def slot(core_):
        return ag.at[pl.ds(y * 16 + zl * 2 + core_, 1)]

    ag[pl.ds(y * 16 + zl * 2 + core, 1), :] = unit
    z_copies = []
    for n, (d, o) in enumerate([(d, o) for d in (0,) + ZSTEPS for o in (0, 1) if d or o]):
        copy = remote(slot(core), slot(core), send_sem.at[12 + n], recv_sem.at[12 + n], z_peer(d, o))
        copy.start()
        z_copies.append(copy)

    wide = [jnp.broadcast_to(value, (1, PX)) for value in res]
    wide_x = [jnp.broadcast_to(value, (1, PX)) for value in answer]

    def finish(layer, faces):
        for c in range(COMP):
            a0, a1, a2, a3 = v0[c, layer + H], v1[c, layer + H], v2[c, layer + H], v3[c, layer]
            sol[c, layer] = wide_x[0] * a0 + wide_x[1] * a1 + wide_x[2] * a2
            left = (wide[0] * a0 + wide[1] * a1) + (wide[2] * a2 + wide[3] * a3)
            place = c * CZ + layer
            faces = jnp.where(lane == place, pltpu.roll(left, place + 1, 1), faces)
            faces = jnp.where(lane == place + 32, pltpu.roll(left, place + 32, 1), faces)
        return faces

    faces = lax.fori_loop(0, CZ, finish, jnp.zeros((PY, PX), jnp.float32))
    store_sol = pltpu.make_async_copy(sol, sol_hbm, local_sem.at[6])
    store_sol.start()
    faces = jnp.transpose(jnp.concatenate([faces, jnp.zeros((PX - PY, PX), jnp.float32)], axis=0))
    left_out[...] = faces[32:64, :]
    left_copy = remote(left_out, left_in, send_sem.at[30], recv_sem.at[30], sub_prev)
    left_copy.start()

    for copy in z_copies:
        copy.wait()
    y_copies = []
    mine = ag.at[pl.ds(y * 16, 12)]
    for k in range(1, NY):
        copy = remote(mine, mine, send_sem.at[22 + k], recv_sem.at[22 + k], y_peer(k))
        copy.start()
        y_copies.append(copy)
    load_inv.wait()
    left_copy.wait()
    summed = faces[0:32, :] + left_in[...]
    for copy in y_copies:
        copy.wait()

    lane8 = lax.broadcasted_iota(jnp.int32, (8, PX), 1)
    row8 = lax.broadcasted_iota(jnp.int32, (8, PX), 0)
    even = [ag[pl.ds(k * 2, NY, stride=16), :] for k in range(NZL)]
    odd = [ag[pl.ds(k * 2 + 1, NY, stride=16), :] for k in range(NZL)]
    turned_even = [pltpu.roll(value, NY - 1, 0) for value in even]
    acc = jnp.zeros((KC, PX), jnp.float32)
    for k in range(NZL):
        after = jnp.where(row8 == NY - 1, turned_even[(k + 1) % NZL], turned_even[k])
        block = jnp.where(lane8 < 64, even[k], after) + pltpu.roll(odd[k], 64, 1)
        for at in range(NY):
            column = (k * NY + at) * PX
            acc = acc + cinv[:, column : column + PX] * block[at : at + 1, :]
    coarse = jnp.sum(acc, axis=1, keepdims=True)
    spots = row * PY + lane
    for j in range(KC):
        hit = (spots == ci_own[0, j]) & (lane < PY)
        summed = summed + jnp.where(hit, coarse[j : j + 1, :], 0.0)
    for c in range(COMP):
        face[0, c] = summed[c * CZ : (c + 1) * CZ, 0:PY]
    store_face = pltpu.make_async_copy(face, face_hbm, local_sem.at[7])
    store_face.start()
    store_sol.wait()
    store_face.wait()


def on_device(body_load, materials, material_tables, corner_index, coarse_inverse):
    f32, i32 = jnp.float32, jnp.int32
    anywhere = pl.BlockSpec(memory_space=pl.ANY)
    return pl.pallas_call(
        kernel,
        out_shape=(
            jax.ShapeDtypeStruct((COMP, CZ, PY, PX), f32),
            jax.ShapeDtypeStruct((1, COMP, CZ, PY), f32),
        ),
        in_specs=[anywhere, anywhere, pl.BlockSpec(memory_space=pltpu.SMEM), anywhere, anywhere],
        out_specs=(anywhere, anywhere),
        scratch_shapes=[
            pltpu.VMEM((COMP, EXT, PY, PX), f32),
            pltpu.VMEM((COMP, EXT, PY, PX), f32),
            pltpu.VMEM((COMP, EXT, PY, PX), f32),
            pltpu.VMEM((COMP, CZ, PY, PX), f32),
            pltpu.VMEM((EXT, PY, PX), i32),
            pltpu.VMEM((COMP * COMP, EXT, PY, PX), f32),
            pltpu.VMEM((KC, N_SUB * N_IN * KC), f32),
            pltpu.VMEM((COMP, CZ, PY, PX), f32),
            pltpu.VMEM((PX, PX), f32),
            pltpu.VMEM((1, PX), f32),
            pltpu.VMEM((N_IN, PX), f32),
            pltpu.VMEM((NY * 16, PX), f32),
            pltpu.VMEM((PY, PX), f32),
            pltpu.VMEM((PY, PX), f32),
            pltpu.VMEM((1, COMP, CZ, PY), f32),
            pltpu.VMEM((1, KC), i32),
            pltpu.VMEM((1, KC), i32),
            pltpu.SMEM((1, KC), i32),
            pltpu.SMEM((1, KC), i32),
            pltpu.SemaphoreType.DMA((8,)),
            pltpu.SemaphoreType.DMA((31,)),
            pltpu.SemaphoreType.DMA((31,)),
        ],
        compiler_params=pltpu.CompilerParams(collective_id=0, has_side_effects=True),
    )(body_load, materials, material_tables, corner_index.reshape(1, KC), coarse_inverse)


def solution(mesh):
    return jax.shard_map(
        on_device,
        mesh=mesh,
        in_specs=(
            P(None, "in", None, "sub"),
            P("in", None, "sub"),
            P(),
            P(("sub", "in")),
            P(("sub", "in"), None),
        ),
        out_specs=(P(None, "in", None, "sub"), P("sub", None, "in", None)),
        check_vma=False,
    )
```

```python
import jax
import jax.numpy as jnp
from jax import lax
from jax.experimental import pallas as pl
from jax.experimental.pallas import tpu as pltpu
from jax.sharding import PartitionSpec as P

MESH = pl.DeviceIdType.MESH
COMP, NMAT, ITERS = 4, 8, 3
CZ, PY, PX, KC = 8, 32, 128, 8
N_SUB, N_IN = 96, 8
H = 1
EXT = CZ + 2 * H
FIRST, LAST, BELOW, ABOVE = H, H + CZ - 1, 0, H + CZ
NY, NZL = 8, 6
PAIRS = [(0, 0), (0, 1), (0, 2), (0, 3), (1, 1), (1, 2), (1, 3), (2, 2), (2, 3)]
ZSTEPS = (1, 2, 3, 10, 11)


def remote(src, dst, send, recv, device):
    return pltpu.make_async_remote_copy(
        src_ref=src, dst_ref=dst, send_sem=send, recv_sem=recv, device_id=device, device_id_type=MESH
    )


def kernel(
    b_hbm, m_hbm, tab_hbm, ci_hbm, cinv_hbm,
    sol_out, face_out,
    v0, v1, v2, v3, mat, gains, w1_low, w1_high, w2_low, pack_out, pack_in,
    cinv, rows, send_row, ex, ag, left_out, left_in,
    ci_vec, ci_left_vec, ci_own, ci_left, tab, local_sem, send_sem, recv_sem,
):
    sub, inn = lax.axis_index("sub"), lax.axis_index("in")
    core, y, zl = sub % 2, (sub // 2) % NY, sub // (2 * NY)
    x, z = inn // 2, (inn % 2) * NZL + zl

    def device(core_, y_, z_):
        return {"sub": ((z_ % NZL) * NY + y_) * 2 + core_, "in": x * 2 + z_ // NZL}

    def in_peer(k):
        return {"sub": sub, "in": (inn + k) % N_IN}

    def z_peer(d, other):
        return device((core + other) % 2, y, (z + d) % (2 * NZL))

    def y_peer(k):
        return device(core, (y + k) % NY, z)

    sub_next = {"sub": (sub + 1) % N_SUB, "in": inn}
    sub_prev = {"sub": (sub + N_SUB - 1) % N_SUB, "in": inn}

    barrier = pltpu.get_barrier_semaphore()
    greet = [in_peer(k) for k in (1, N_IN - 1)]
    greet += [in_peer(k) for k in range(2, N_IN - 1)]
    greet += [z_peer(d, o) for d in (0, 1, 2, 3, 9, 10, 11) for o in (0, 1) if d or o]
    greet += [y_peer(k) for k in range(1, NY)]
    greet += [sub_next, sub_prev]
    for peer in greet:
        pl.semaphore_signal(barrier, inc=1, device_id=peer, device_id_type=MESH)

    load_b = pltpu.make_async_copy(b_hbm, v0.at[:, pl.ds(H, CZ)], local_sem.at[0])
    load_m = pltpu.make_async_copy(m_hbm, mat.at[pl.ds(H, CZ)], local_sem.at[1])
    load_t = pltpu.make_async_copy(tab_hbm, tab, local_sem.at[6])
    load_c = pltpu.make_async_copy(ci_hbm, ci_vec, local_sem.at[2])
    load_inv = pltpu.make_async_copy(cinv_hbm, cinv, local_sem.at[3])
    load_own = pltpu.make_async_copy(ci_hbm, ci_own, local_sem.at[4])
    for load in (load_b, load_m, load_t, load_c, load_own, load_inv):
        load.start()
    load_t.wait()

    low, high = None, None
    for k in range(NMAT):
        for c in range(COMP):
            centre = tab[c, c, k]
            radius = jnp.float32(6.0)
            for d in range(COMP):
                if d != c:
                    radius = radius + jnp.maximum(tab[c, d, k], -tab[c, d, k])
            lo, hi = centre - radius, centre + radius
            low = lo if low is None else jnp.minimum(low, lo)
            high = hi if high is None else jnp.maximum(high, hi)
    sigma = 6.0 + 0.5 * (low + high)
    width = 0.5 * (high - low)
    inv_row = 1.0 / jnp.full((1, PX), width, jnp.float32)
    shift = 6.0 - sigma
    keep_low = jnp.where(inn > 0, jnp.float32(1.0), jnp.float32(0.0))
    keep_high = jnp.where(inn < N_IN - 1, jnp.float32(1.0), jnp.float32(0.0))
    cross = -inv_row
    cross_low, cross_high = cross * keep_low, cross * keep_high

    load_b.wait()
    load_m.wait()
    load_c.wait()
    load_own.wait()
    pl.semaphore_wait(barrier, len(greet))

    up, down = in_peer(1), in_peer(N_IN - 1)
    send_b_up = remote(v0.at[:, LAST], v0.at[:, BELOW], send_sem.at[0], recv_sem.at[0], up)
    send_b_down = remote(v0.at[:, FIRST], v0.at[:, ABOVE], send_sem.at[1], recv_sem.at[1], down)
    send_m_down = remote(mat.at[FIRST], mat.at[ABOVE], send_sem.at[2], recv_sem.at[2], down)
    send_w1_up = remote(w1_high, v1.at[:, BELOW], send_sem.at[3], recv_sem.at[3], up)
    send_w1_down = remote(w1_low, v1.at[:, ABOVE], send_sem.at[4], recv_sem.at[4], down)
    send_w2_down = remote(w2_low, v2.at[:, ABOVE], send_sem.at[5], recv_sem.at[5], down)
    send_pack_up = remote(pack_out, pack_in, send_sem.at[6], recv_sem.at[6], up)
    send_ci = remote(ci_vec, ci_left_vec, send_sem.at[7], recv_sem.at[7], sub_next)
    halos = (send_b_up, send_b_down, send_m_down, send_w1_up, send_w1_down, send_w2_down, send_pack_up, send_ci)
    for copy in (send_b_down, send_b_up, send_m_down, send_ci):
        copy.start()

    lane = lax.broadcasted_iota(jnp.int32, (PY, PX), 1)
    row = lax.broadcasted_iota(jnp.int32, (PY, PX), 0)

    def tables_of(layer, ids=None):
        ids = mat[layer] if ids is None else ids
        top, mid, bottom = ids >= 4, (ids & 2) != 0, (ids & 1) != 0
        for c in range(COMP):
            for d in range(COMP):
                pairs = [jnp.where(bottom, tab[c, d, 2 * k + 1], tab[c, d, 2 * k]) for k in range(4)]
                value = jnp.where(top, jnp.where(mid, pairs[3], pairs[2]), jnp.where(mid, pairs[1], pairs[0]))
                gains[c * COMP + d, layer] = value + shift if c == d else value

    def within(centre, layer):
        result = []
        for c in range(COMP):
            v = centre[c]
            beside = jnp.where(row == 0, 0.0, pltpu.roll(v, 1, 0))
            beside = beside + jnp.where(row == PY - 1, 0.0, pltpu.roll(v, PY - 1, 0))
            beside = beside + jnp.where(lane == 0, 0.0, pltpu.roll(v, 1, 1))
            beside = beside + jnp.where(lane == PX - 1, 0.0, pltpu.roll(v, PX - 1, 1))
            coupled = gains[c * COMP, layer] * centre[0]
            for d in range(1, COMP):
                coupled = coupled + gains[c * COMP + d, layer] * centre[d]
            result.append(coupled - beside)
        return result

    def take(src, layer):
        return [src[c, layer] for c in range(COMP)]

    def put(dst, layer, values):
        for c in range(COMP):
            dst[c, layer] = values[c]

    def apply_at(src, layer, below=True, above=True):
        centre = take(src, layer)
        result = within(centre, layer)
        for c in range(COMP):
            if below:
                result[c] = result[c] - src[c, layer - 1]
            if above:
                result[c] = result[c] - src[c, layer + 1]
        return centre, [value * inv_row for value in result]

    def layers(lo, hi, body):
        @pl.loop(lo, hi)
        def _(layer):
            body(layer)

    def products(sums, basis):
        out = []
        for (i, j), total in zip(PAIRS, sums):
            part = basis[i][0] * basis[j][0]
            for c in range(1, COMP):
                part = part + basis[i][c] * basis[j][c]
            out.append(total + ((part[0:8] + part[8:16]) + (part[16:24] + part[24:32])))
        return tuple(out)

    def third(layer, sums, below=True):
        a2, a3 = apply_at(v2, layer, below=below)
        put(v3, layer - H, a3)
        return products(sums, (take(v0, layer), take(v1, layer), a2, a3))

    def across(sums):
        mine = [cross_high * value for value in take(v2, LAST)]
        out = list(sums)
        for i, source in enumerate((v0, v1, v2)):
            part = source[0, ABOVE] * mine[0]
            for c in range(1, COMP):
                part = part + source[c, ABOVE] * mine[c]
            n = PAIRS.index((i, 3))
            out[n] = out[n] + ((part[0:8] + part[8:16]) + (part[16:24] + part[24:32]))
        return tuple(out)

    def first(layer):
        put(v1, layer, apply_at(v0, layer)[1])

    def second(layer):
        put(v2, layer, apply_at(v1, layer)[1])

    layers(FIRST, FIRST + 2, tables_of)
    layers(LAST - 1, LAST + 1, tables_of)
    low1 = apply_at(v0, FIRST, below=False)[1]
    put(v1, FIRST, low1)
    high1 = apply_at(v0, LAST, above=False)[1]
    put(v1, LAST, high1)
    for c in range(COMP):
        w1_low[c] = low1[c]
        w1_high[c] = high1[c]
    send_w1_down.start()
    send_w1_up.start()
    first(FIRST + 1)
    first(LAST - 1)
    low2 = apply_at(v1, FIRST, below=False)[1]
    for c in range(COMP):
        w2_low[c] = low2[c]
    send_w2_down.start()
    high2 = apply_at(v1, LAST, above=False)[1]
    packed = jnp.zeros((PY, PX), jnp.float32)
    for c, value in enumerate(high2 + [mat[LAST].astype(jnp.float32)]):
        packed = jnp.where(lane == c, pltpu.roll(value, c + 1, 1), packed)
        packed = jnp.where(lane == 8 + c, pltpu.roll(value, 8 + c, 1), packed)
    pack_out[...] = packed
    send_pack_up.start()

    layers(FIRST + 2, LAST - 1, tables_of)
    layers(FIRST + 2, LAST - 1, first)
    layers(FIRST + 2, LAST - 1, second)
    sums = tuple(jnp.zeros((8, PX), jnp.float32) for _ in PAIRS)
    sums = lax.fori_loop(FIRST + 3, LAST - 2, third, sums)

    send_b_down.wait_recv()
    send_m_down.wait_recv()
    send_b_up.wait_recv()
    send_ci.wait()
    load_left = pltpu.make_async_copy(ci_left_vec, ci_left, local_sem.at[5])
    load_left.start()
    for c in range(COMP):
        v1[c, FIRST] = v1[c, FIRST] + cross_low * v0[c, BELOW]
        v1[c, LAST] = v1[c, LAST] + cross_high * v0[c, ABOVE]
    tables_of(ABOVE)
    second(FIRST + 1)
    second(LAST - 1)
    send_w1_down.wait_recv()
    send_w1_up.wait_recv()
    for c in range(COMP):
        v1[c, BELOW] = keep_low * v1[c, BELOW] + cross_low * v0[c, FIRST]
        v1[c, ABOVE] = keep_high * v1[c, ABOVE] + cross_high * v0[c, LAST]
    second(FIRST)
    second(LAST)
    sums = lax.fori_loop(FIRST + 1, FIRST + 3, third, sums)
    sums = lax.fori_loop(LAST - 2, LAST, third, sums)
    above = within(take(v0, LAST), ABOVE)
    above = [term * inv_row + v1[c, LAST] for c, term in enumerate(above)]
    sums = third(FIRST, sums, below=False)
    load_left.wait()
    send_w2_down.wait_recv()
    for c in range(COMP):
        v2[c, ABOVE] = keep_high * v2[c, ABOVE] + cross_high * above[c]
    sums = third(LAST, sums)
    sums = across(sums)
    send_pack_up.wait_recv()
    packed = pack_in[...]

    def column(c):
        return jnp.where(lane == PX - 1, pltpu.roll(packed, PX - 1 - c, 1), pltpu.roll(packed, PX - 8 - c, 1))

    at_ends = (lane == 0) | (lane == PX - 1)
    tables_of(BELOW, jnp.where(at_ends, column(COMP), 0.0).astype(jnp.int32))
    below = within(take(v0, FIRST), BELOW)
    for c in range(COMP):
        value = keep_low * column(c) + cross_low * (below[c] * inv_row + v1[c, FIRST])
        v3[c, 0] = v3[c, 0] + cross_low * jnp.where(at_ends, value, 0.0)

    for j in range(KC):
        for side, ids in ((0, ci_own), (1, ci_left)):
            spot = ids[0, j]
            c, layer, at = spot // (CZ * PY), (spot // PY) % CZ, spot % PY
            place = side * KC + j
            rows[pl.ds(place, 1), :] = v0[c, layer + H, pl.ds(at, 1), :]
            rows[pl.ds(16 + place, 1), :] = v1[c, layer + H, pl.ds(at, 1), :]
            rows[pl.ds(32 + place, 1), :] = v2[c, layer + H, pl.ds(at, 1), :]
            rows[pl.ds(48 + place, 1), :] = v3[c, layer, pl.ds(at, 1), :]
    rows[pl.ds(64, 64), :] = jnp.zeros((64, PX), jnp.float32)
    turned = jnp.transpose(rows[...])
    lane1 = lax.broadcasted_iota(jnp.int32, (1, PX), 1)
    own_row = jnp.where((lane1 // KC) % 2 == 0, turned[PX - 1 : PX, :], turned[0:1, :])
    own_row = jnp.where(lane1 < 64, own_row, 0.0)
    for n, total in enumerate(sums):
        whole = jnp.sum(jnp.sum(total, axis=0, keepdims=True), axis=1, keepdims=True)
        own_row = jnp.where(lane1 == 64 + n, whole, own_row)
    send_row[...] = own_row
    ex[pl.ds(inn, 1), :] = own_row
    for k in range(1, N_IN):
        remote(send_row, ex.at[pl.ds(inn, 1)], send_sem.at[8], recv_sem.at[8], in_peer(k)).start()
    everything = ex.at[pl.ds(0, N_IN - 1)]
    remote(everything, everything, send_sem.at[8], recv_sem.at[8], in_peer(1)).wait()

    everyone = ex[...]
    total = jnp.sum(everyone, axis=0, keepdims=True)
    gram = {}
    for n, (i, j) in enumerate(PAIRS):
        value = jnp.sum(jnp.where(lane1 == 64 + n, total, 0.0), axis=1, keepdims=True)
        gram[i, j] = gram[j, i] = value

    def form(p, q, offset):
        value = None
        for i, a in enumerate(p):
            for j, b in enumerate(q):
                term = a * b * gram[i, j + offset]
                value = term if value is None else value + term
        return value

    res = [jnp.ones((1, 1), jnp.float32)]
    direction, previous = list(res), []
    rr = form(res, res, 0)
    dd, beta = rr, None
    answer = [jnp.zeros((1, 1), jnp.float32) for _ in range(ITERS)]
    for step in range(ITERS):
        delta = width * form(direction, direction, 1)
        if step:
            delta = delta + sigma * (beta * beta * dd_before)
        inverse = 1.0 / (sigma * rr + delta)
        alpha = rr * inverse
        for j, value in enumerate(direction):
            answer[j] = answer[j] + alpha * value
        moved = []
        for j in range(step + 2):
            value = None
            if j <= step:
                value = res[j] * delta
                if j < len(previous):
                    value = value - sigma * rr * (beta * previous[j])
                value = value * inverse
            if j:
                part = (alpha * width) * direction[j - 1]
                value = -part if value is None else value - part
            moved.append(value)
        if step + 1 < ITERS:
            new = form(moved, moved, 0)
            beta = new / rr
            previous = direction
            direction = [
                value + beta * direction[j] if j <= step else value for j, value in enumerate(moved)
            ]
            dd_before = dd
            dd = new + beta * beta * dd
            rr = new
        res = moved

    factors = jnp.zeros((1, PX), jnp.float32)
    for k in range(ITERS + 1):
        factors = jnp.where(lane1 // 16 == k, res[k], factors)
    mixed = everyone * factors
    mixed = (mixed + pltpu.roll(mixed, PX - 16, 1)) + (pltpu.roll(mixed, PX - 32, 1) + pltpu.roll(mixed, PX - 48, 1))
    unit = jnp.zeros((1, PX), jnp.float32)
    for i in range(N_IN):
        piece = mixed[i : i + 1, :]
        piece = jnp.where(lane1 < 8, piece, 0.0) + pltpu.roll(jnp.where((lane1 >= 8) & (lane1 < 16), piece, 0.0), 56, 1)
        unit = unit + (pltpu.roll(piece, KC * i, 1) if i else piece)

    spot_row = y * 16 + zl * 2 + core
    ag[pl.ds(spot_row, 1), :] = unit
    mine = ag.at[pl.ds(spot_row, 1)]
    z_peers = [z_peer(d, o) for d in (0,) + ZSTEPS for o in (0, 1) if d or o]
    for peer in z_peers:
        remote(mine, mine, send_sem.at[9], recv_sem.at[9], peer).start()

    wide = [jnp.broadcast_to(value, (1, PX)) for value in res]
    wide_x = [jnp.broadcast_to(value, (1, PX)) for value in answer]

    def finish(layer, faces):
        for c in range(COMP):
            a0, a1, a2, a3 = v0[c, layer + H], v1[c, layer + H], v2[c, layer + H], v3[c, layer]
            sol_out[c, layer] = wide_x[0] * a0 + wide_x[1] * a1 + wide_x[2] * a2
            left = (wide[0] * a0 + wide[1] * a1) + (wide[2] * a2 + wide[3] * a3)
            place = c * CZ + layer
            faces = jnp.where(lane == place, pltpu.roll(left, place + 1, 1), faces)
            faces = jnp.where(lane == place + 32, pltpu.roll(left, place + 32, 1), faces)
        return faces

    faces = lax.fori_loop(0, CZ, finish, jnp.zeros((PY, PX), jnp.float32))
    faces = jnp.transpose(jnp.concatenate([faces, jnp.zeros((PX - PY, PX), jnp.float32)], axis=0))
    left_out[...] = faces[32:64, :]
    left_copy = remote(left_out, left_in, send_sem.at[11], recv_sem.at[11], sub_prev)
    left_copy.start()

    arrived = ag.at[pl.ds(0, len(z_peers))]
    remote(arrived, arrived, send_sem.at[9], recv_sem.at[9], in_peer(1)).wait()
    mine = ag.at[pl.ds(y * 16, 12)]
    for k in range(1, NY):
        remote(mine, mine, send_sem.at[10], recv_sem.at[10], y_peer(k)).start()
    load_inv.wait()
    left_copy.wait()
    summed = faces[0:32, :] + left_in[...]
    for copy in halos[:-1]:
        copy.wait_send()
    arrived = ag.at[pl.ds(0, 12 * (NY - 1))]
    remote(arrived, arrived, send_sem.at[10], recv_sem.at[10], in_peer(1)).wait()

    lane8 = lax.broadcasted_iota(jnp.int32, (8, PX), 1)
    row8 = lax.broadcasted_iota(jnp.int32, (8, PX), 0)
    even = [ag[pl.ds(k * 2, NY, stride=16), :] for k in range(NZL)]
    odd = [ag[pl.ds(k * 2 + 1, NY, stride=16), :] for k in range(NZL)]
    turned_even = [pltpu.roll(value, NY - 1, 0) for value in even]
    acc = jnp.zeros((KC, PX), jnp.float32)
    for k in range(NZL):
        after = jnp.where(row8 == NY - 1, turned_even[(k + 1) % NZL], turned_even[k])
        block = jnp.where(lane8 < 64, even[k], after) + pltpu.roll(odd[k], 64, 1)
        for at in range(NY):
            column = (k * NY + at) * PX
            acc = acc + cinv[:, column : column + PX] * block[at : at + 1, :]
    coarse = jnp.sum(acc, axis=1, keepdims=True)
    spots = row * PY + lane
    for j in range(KC):
        hit = (spots == ci_own[0, j]) & (lane < PY)
        summed = summed + jnp.where(hit, coarse[j : j + 1, :], 0.0)
    for c in range(COMP):
        face_out[0, c] = summed[c * CZ : (c + 1) * CZ, 0:PY]


def on_device(body_load, materials, material_tables, corner_index, coarse_inverse):
    f32, i32 = jnp.float32, jnp.int32
    anywhere = pl.BlockSpec(memory_space=pl.ANY)
    vmem = pl.BlockSpec(memory_space=pltpu.VMEM)
    layer = (COMP, PY, PX)
    return pl.pallas_call(
        kernel,
        out_shape=(
            pltpu.VMEM((COMP, CZ, PY, PX), f32),
            pltpu.VMEM((1, COMP, CZ, PY), f32),
        ),
        in_specs=[anywhere] * 5,
        out_specs=(vmem, vmem),
        scratch_shapes=[
            pltpu.VMEM((COMP, EXT, PY, PX), f32),
            pltpu.VMEM((COMP, EXT, PY, PX), f32),
            pltpu.VMEM((COMP, EXT, PY, PX), f32),
            pltpu.VMEM((COMP, CZ, PY, PX), f32),
            pltpu.VMEM((EXT, PY, PX), i32),
            pltpu.VMEM((COMP * COMP, EXT, PY, PX), f32),
            pltpu.VMEM(layer, f32),
            pltpu.VMEM(layer, f32),
            pltpu.VMEM(layer, f32),
            pltpu.VMEM((PY, PX), f32),
            pltpu.VMEM((PY, PX), f32),
            pltpu.VMEM((KC, N_SUB * N_IN * KC), f32),
            pltpu.VMEM((PX, PX), f32),
            pltpu.VMEM((1, PX), f32),
            pltpu.VMEM((N_IN, PX), f32),
            pltpu.VMEM((NY * 16, PX), f32),
            pltpu.VMEM((PY, PX), f32),
            pltpu.VMEM((PY, PX), f32),
            pltpu.VMEM((1, KC), i32),
            pltpu.VMEM((1, KC), i32),
            pltpu.SMEM((1, KC), i32),
            pltpu.SMEM((1, KC), i32),
            pltpu.SMEM((COMP, COMP, NMAT), f32),
            pltpu.SemaphoreType.DMA((7,)),
            pltpu.SemaphoreType.DMA((12,)),
            pltpu.SemaphoreType.DMA((12,)),
        ],
        compiler_params=pltpu.CompilerParams(collective_id=0, has_side_effects=True),
    )(
        body_load,
        materials,
        jnp.transpose(material_tables, (1, 2, 0)),
        corner_index.reshape(1, KC),
        coarse_inverse,
    )


def solution(mesh):
    return jax.shard_map(
        on_device,
        mesh=mesh,
        in_specs=(
            P(None, "in", None, "sub"),
            P("in", None, "sub"),
            P(),
            P(("sub", "in")),
            P(("sub", "in"), None),
        ),
        out_specs=(P(None, "in", None, "sub"), P("sub", None, "in", None)),
        check_vma=False,
    )
```

```python
import jax
import jax.numpy as jnp
from jax import lax
from jax.experimental import pallas as pl
from jax.experimental.pallas import tpu as pltpu
from jax.sharding import PartitionSpec as P

MESH = pl.DeviceIdType.MESH
COMP, NMAT, ITERS = 4, 8, 3
CZ, PY, PX, KC = 8, 32, 128, 8
N_SUB, N_IN = 96, 8
H = 1
EXT = CZ + 2 * H
FIRST, LAST, BELOW, ABOVE = H, H + CZ - 1, 0, H + CZ
NX_CHIPS, NY, NZL = 4, 8, 6
PAIRS = [(0, 0), (0, 1), (0, 2), (0, 3), (1, 1), (1, 2), (1, 3), (2, 2), (2, 3)]


def remote(src, dst, send, recv, device):
    return pltpu.make_async_remote_copy(
        src_ref=src, dst_ref=dst, send_sem=send, recv_sem=recv, device_id=device, device_id_type=MESH
    )


def kernel(
    b_hbm, m_hbm, tab_hbm, ci_hbm, cinv_hbm,
    sol_out, face_out,
    v0, v1, v2, v3, relay, mat, gains, w1_low, w1_high, w2_low, w2_in, pack_out, pack_in,
    cinv, rows, send_row, ex, ag, left_out, left_in,
    ci_vec, ci_left_vec, ci_own, ci_left, tab, local_sem, send_sem, recv_sem,
):
    sub, inn = lax.axis_index("sub"), lax.axis_index("in")
    core, y, zl = sub % 2, (sub // 2) % NY, sub // (2 * NY)
    x, z = inn // 2, (inn % 2) * NZL + zl

    def in_peer(k):
        return {"sub": sub, "in": (inn + k) % N_IN}

    def plane_peer(dx, dz):
        z_ = (z + dz) % (2 * NZL)
        return {"sub": ((z_ % NZL) * NY + y) * 2 + core, "in": ((x + dx) % NX_CHIPS) * 2 + z_ // NZL}

    def y_peer(k, other):
        return {"sub": (zl * NY + (y + k) % NY) * 2 + (core + other) % 2, "in": inn}

    sub_next = {"sub": (sub + 1) % N_SUB, "in": inn}
    sub_prev = {"sub": (sub + N_SUB - 1) % N_SUB, "in": inn}

    barrier = pltpu.get_barrier_semaphore()
    greet = [in_peer(1), in_peer(N_IN - 1)]
    greet += [plane_peer(dx, dz) for dz in range(2 * NZL) for dx in range(NX_CHIPS) if dx or dz]
    greet += [y_peer(k, o) for k in range(NY) for o in (0, 1) if k or o]
    greet += [sub_next, sub_prev]
    for peer in greet:
        pl.semaphore_signal(barrier, inc=1, device_id=peer, device_id_type=MESH)

    load_b = pltpu.make_async_copy(b_hbm, v0.at[:, pl.ds(H, CZ)], local_sem.at[0])
    load_m = pltpu.make_async_copy(m_hbm, mat.at[pl.ds(H, CZ)], local_sem.at[1])
    load_t = pltpu.make_async_copy(tab_hbm, tab, local_sem.at[6])
    load_c = pltpu.make_async_copy(ci_hbm, ci_vec, local_sem.at[2])
    load_inv = pltpu.make_async_copy(cinv_hbm, cinv, local_sem.at[3])
    load_own = pltpu.make_async_copy(ci_hbm, ci_own, local_sem.at[4])
    for load in (load_b, load_m, load_t, load_c, load_own, load_inv):
        load.start()
    load_t.wait()

    low, high = None, None
    for k in range(NMAT):
        for c in range(COMP):
            centre = tab[c, c, k]
            radius = jnp.float32(6.0)
            for d in range(COMP):
                if d != c:
                    radius = radius + jnp.maximum(tab[c, d, k], -tab[c, d, k])
            lo, hi = centre - radius, centre + radius
            low = lo if low is None else jnp.minimum(low, lo)
            high = hi if high is None else jnp.maximum(high, hi)
    sigma = 6.0 + 0.5 * (low + high)
    width = 0.5 * (high - low)
    inv_row = 1.0 / jnp.full((1, PX), width, jnp.float32)
    shift = 6.0 - sigma
    keep_low = jnp.where(inn > 0, jnp.float32(1.0), jnp.float32(0.0))
    keep_high = jnp.where(inn < N_IN - 1, jnp.float32(1.0), jnp.float32(0.0))
    cross = -inv_row
    cross_low, cross_high = cross * keep_low, cross * keep_high

    load_b.wait()
    load_m.wait()
    load_c.wait()
    load_own.wait()
    pl.semaphore_wait(barrier, len(greet))

    up, down = in_peer(1), in_peer(N_IN - 1)
    send_b_up = remote(v0.at[:, LAST], v0.at[:, BELOW], send_sem.at[0], recv_sem.at[0], up)
    send_b_down = remote(v0.at[:, FIRST], v0.at[:, ABOVE], send_sem.at[1], recv_sem.at[1], down)
    send_m_down = remote(mat.at[FIRST], mat.at[ABOVE], send_sem.at[2], recv_sem.at[2], down)
    send_w1_up = remote(w1_high, v1.at[:, BELOW], send_sem.at[3], recv_sem.at[3], up)
    send_w1_down = remote(w1_low, v1.at[:, ABOVE], send_sem.at[4], recv_sem.at[4], down)
    send_w2_down = remote(w2_low, w2_in, send_sem.at[5], recv_sem.at[5], down)
    send_pack_up = remote(pack_out, pack_in, send_sem.at[6], recv_sem.at[6], up)
    send_ci = remote(ci_vec, ci_left_vec, send_sem.at[7], recv_sem.at[7], sub_next)
    up_relayed, up_via, down_relayed, down_via = N_IN - 3, N_IN - 1, 2, 0
    has_up, has_down = inn < N_IN - 1, inn > 0

    def to(index):
        return {"sub": sub, "in": index}

    relay_up = remote(v0.at[:, LAST], relay, send_sem.at[0], recv_sem.at[11], to(up_via))
    relay_down = remote(v0.at[:, FIRST], relay, send_sem.at[1], recv_sem.at[11], to(down_via))
    pass_up = remote(relay, v0.at[:, BELOW], send_sem.at[11], recv_sem.at[0], to(up_relayed + 1))
    pass_down = remote(relay, v0.at[:, ABOVE], send_sem.at[11], recv_sem.at[1], to(down_relayed - 1))
    pl.when(inn == down_relayed)(relay_down.start)
    pl.when(inn == up_relayed)(relay_up.start)
    pl.when(has_down & (inn != down_relayed))(send_b_down.start)
    pl.when(has_up & (inn != up_relayed))(send_b_up.start)
    pl.when(has_down)(send_m_down.start)
    send_ci.start()

    @pl.when(inn == 0)
    def _():
        for c in range(COMP):
            v0[c, BELOW] = jnp.zeros((PY, PX), jnp.float32)
            v1[c, BELOW] = jnp.zeros((PY, PX), jnp.float32)
        pack_in[...] = jnp.zeros((16, PX), jnp.float32)

    @pl.when(inn == N_IN - 1)
    def _():
        mat[ABOVE] = jnp.zeros((PY, PX), jnp.int32)
        for c in range(COMP):
            v0[c, ABOVE] = jnp.zeros((PY, PX), jnp.float32)
            v1[c, ABOVE] = jnp.zeros((PY, PX), jnp.float32)
            w2_in[c] = jnp.zeros((PY, PX), jnp.float32)

    lane = lax.broadcasted_iota(jnp.int32, (PY, PX), 1)
    row = lax.broadcasted_iota(jnp.int32, (PY, PX), 0)

    def tables_of(layer, ids=None):
        ids = mat[layer] if ids is None else ids
        top, mid, bottom = ids >= 4, (ids & 2) != 0, (ids & 1) != 0
        for c in range(COMP):
            for d in range(COMP):
                pairs = [jnp.where(bottom, tab[c, d, 2 * k + 1], tab[c, d, 2 * k]) for k in range(4)]
                value = jnp.where(top, jnp.where(mid, pairs[3], pairs[2]), jnp.where(mid, pairs[1], pairs[0]))
                gains[c * COMP + d, layer] = value + shift if c == d else value

    def within(centre, layer):
        result = []
        for c in range(COMP):
            v = centre[c]
            beside = jnp.where(row == 0, 0.0, pltpu.roll(v, 1, 0))
            beside = beside + jnp.where(row == PY - 1, 0.0, pltpu.roll(v, PY - 1, 0))
            beside = beside + jnp.where(lane == 0, 0.0, pltpu.roll(v, 1, 1))
            beside = beside + jnp.where(lane == PX - 1, 0.0, pltpu.roll(v, PX - 1, 1))
            coupled = gains[c * COMP, layer] * centre[0]
            for d in range(1, COMP):
                coupled = coupled + gains[c * COMP + d, layer] * centre[d]
            result.append(coupled - beside)
        return result

    def take(src, layer):
        return [src[c, layer] for c in range(COMP)]

    def put(dst, layer, values):
        for c in range(COMP):
            dst[c, layer] = values[c]

    def apply_at(src, layer, below=True, above=True):
        centre = take(src, layer)
        result = within(centre, layer)
        for c in range(COMP):
            if below:
                result[c] = result[c] - src[c, layer - 1]
            if above:
                result[c] = result[c] - src[c, layer + 1]
        return centre, [value * inv_row for value in result]

    def layers(lo, hi, body):
        @pl.loop(lo, hi)
        def _(layer):
            body(layer)

    def products(sums, basis, only=None):
        out = []
        for (i, j), total in zip(PAIRS, sums):
            if basis[j] is None or only not in (None, j):
                out.append(total)
                continue
            part = basis[i][0] * basis[j][0]
            for c in range(1, COMP):
                part = part + basis[i][c] * basis[j][c]
            out.append(total + ((part[0:8] + part[8:16]) + (part[16:24] + part[24:32])))
        return tuple(out)

    def third(layer, sums, below=True):
        a2, a3 = apply_at(v2, layer, below=below)
        put(v3, layer - H, a3)
        return products(sums, (take(v0, layer), take(v1, layer), a2, a3))

    def across(sums):
        mine = [cross_high * value for value in take(v2, LAST)]
        out = list(sums)
        for i, source in enumerate((v0, v1, v2)):
            part = source[0, ABOVE] * mine[0]
            for c in range(1, COMP):
                part = part + source[c, ABOVE] * mine[c]
            n = PAIRS.index((i, 3))
            out[n] = out[n] + ((part[0:8] + part[8:16]) + (part[16:24] + part[24:32]))
        return tuple(out)

    def first(layer):
        put(v1, layer, apply_at(v0, layer)[1])

    def second(layer):
        put(v2, layer, apply_at(v1, layer)[1])

    layers(FIRST, FIRST + 2, tables_of)
    layers(LAST - 1, LAST + 1, tables_of)
    low1 = apply_at(v0, FIRST, below=False)[1]
    put(v1, FIRST, low1)
    high1 = apply_at(v0, LAST, above=False)[1]
    put(v1, LAST, high1)
    for c in range(COMP):
        w1_low[c] = low1[c]
        w1_high[c] = high1[c]
    pl.when(has_down)(send_w1_down.start)
    pl.when(has_up)(send_w1_up.start)
    first(FIRST + 1)
    first(LAST - 1)
    low2 = apply_at(v1, FIRST, below=False)[1]
    for c in range(COMP):
        w2_low[c] = low2[c]
    pl.when(has_down)(send_w2_down.start)
    high2 = apply_at(v1, LAST, above=False)[1]
    packed = jnp.zeros((PY, PX), jnp.float32)
    for c, value in enumerate(high2 + [mat[LAST].astype(jnp.float32)]):
        packed = jnp.where(lane == c, pltpu.roll(value, c + 1, 1), packed)
        packed = jnp.where(lane == 8 + c, pltpu.roll(value, 8 + c, 1), packed)
    blank = jnp.zeros((PX - PY, PX), jnp.float32)
    pack_out[...] = jnp.transpose(jnp.concatenate([packed, blank], axis=0))[0:16, :]
    pl.when(has_up)(send_pack_up.start)

    layers(FIRST + 2, LAST - 1, tables_of)
    layers(FIRST + 2, LAST - 1, first)
    layers(FIRST + 2, LAST - 1, second)
    sums = tuple(jnp.zeros((8, PX), jnp.float32) for _ in PAIRS)
    sums = lax.fori_loop(FIRST + 3, LAST - 2, third, sums)

    @pl.when(inn == up_via)
    def _():
        relay_up.wait_recv()
        pass_up.start()

    @pl.when(inn == down_via)
    def _():
        relay_down.wait_recv()
        pass_down.start()

    pl.when(has_up)(send_b_down.wait_recv)
    pl.when(has_up)(send_m_down.wait_recv)
    pl.when(has_down)(send_b_up.wait_recv)
    send_ci.wait()
    load_left = pltpu.make_async_copy(ci_left_vec, ci_left, local_sem.at[5])
    load_left.start()
    for c in range(COMP):
        v1[c, FIRST] = v1[c, FIRST] + cross_low * v0[c, BELOW]
        v1[c, LAST] = v1[c, LAST] + cross_high * v0[c, ABOVE]
    tables_of(ABOVE)
    second(FIRST + 1)
    second(LAST - 1)
    pl.when(has_up)(send_w1_down.wait_recv)
    pl.when(has_down)(send_w1_up.wait_recv)
    for c in range(COMP):
        v1[c, BELOW] = keep_low * v1[c, BELOW] + cross_low * v0[c, FIRST]
        v1[c, ABOVE] = keep_high * v1[c, ABOVE] + cross_high * v0[c, LAST]
    second(FIRST)
    second(LAST)
    sums = lax.fori_loop(FIRST + 1, FIRST + 3, third, sums)
    sums = lax.fori_loop(LAST - 2, LAST, third, sums)
    above = within(take(v0, LAST), ABOVE)
    above = [term * inv_row + v1[c, LAST] for c, term in enumerate(above)]
    sums = third(FIRST, sums, below=False)
    load_left.wait()
    pl.when(has_down)(send_pack_up.wait_recv)
    packed = jnp.concatenate([pack_in[...], jnp.zeros((PX - 16, PX), jnp.float32)], axis=0)
    packed = jnp.transpose(packed)[0:PY, :]

    def column(c):
        return jnp.where(lane == PX - 1, pltpu.roll(packed, PX - 1 - c, 1), pltpu.roll(packed, PX - 8 - c, 1))

    at_ends = (lane == 0) | (lane == PX - 1)
    tables_of(BELOW, jnp.where(at_ends, column(COMP), 0.0).astype(jnp.int32))
    below = within(take(v0, FIRST), BELOW)
    for c in range(COMP):
        value = keep_low * column(c) + cross_low * (below[c] * inv_row + v1[c, FIRST])
        v3[c, 0] = v3[c, 0] + cross_low * jnp.where(at_ends, value, 0.0)

    places = []
    for j in range(KC):
        for side, ids in ((0, ci_own), (1, ci_left)):
            spot = ids[0, j]
            c, layer, at = spot // (CZ * PY), (spot // PY) % CZ, spot % PY
            place = side * KC + j
            places.append((place, c, layer, at))
            rows[pl.ds(place, 1), :] = v0[c, layer + H, pl.ds(at, 1), :]
            rows[pl.ds(16 + place, 1), :] = v1[c, layer + H, pl.ds(at, 1), :]
            rows[pl.ds(32 + place, 1), :] = v2[c, layer + H, pl.ds(at, 1), :]
    rows[pl.ds(64, 64), :] = jnp.zeros((64, PX), jnp.float32)
    lane1 = lax.broadcasted_iota(jnp.int32, (1, PX), 1)

    def with_sums(into, chosen):
        for n, (i, j) in enumerate(PAIRS):
            if chosen(j):
                whole = jnp.sum(jnp.sum(sums[n], axis=0, keepdims=True), axis=1, keepdims=True)
                into = jnp.where(lane1 == 64 + n, whole, into)
        return into

    a2 = take(v2, LAST)
    a0, a1 = take(v0, LAST), take(v1, LAST)
    sums = products(sums, (a0, a1, a2, None))
    sums_row = with_sums(jnp.zeros((1, PX), jnp.float32), lambda j: j < 3)
    pl.when(has_up)(send_w2_down.wait_recv)
    for c in range(COMP):
        v2[c, ABOVE] = keep_high * w2_in[c] + cross_high * above[c]
    a3 = apply_at(v2, LAST)[1]
    put(v3, LAST - H, a3)
    sums = products(sums, (a0, a1, a2, a3), only=3)
    sums = across(sums)
    for place, c, layer, at in places:
        rows[pl.ds(48 + place, 1), :] = v3[c, layer, pl.ds(at, 1), :]
    turned = jnp.transpose(rows[...])
    own_row = jnp.where((lane1 // KC) % 2 == 0, turned[PX - 1 : PX, :], turned[0:1, :])
    own_row = jnp.where(lane1 < 64, own_row, with_sums(sums_row, lambda j: j == 3))
    send_row[...] = own_row
    ex[pl.ds(zl * N_IN + inn, 1), :] = own_row
    n_plane = 2 * NZL * NX_CHIPS
    for dz in range(2 * NZL):
        for dx in range(NX_CHIPS):
            if dx or dz:
                spot = ex.at[pl.ds(zl * N_IN + inn, 1)]
                remote(send_row, spot, send_sem.at[8], recv_sem.at[8], plane_peer(dx, dz)).start()
    arrived = ex.at[pl.ds(0, n_plane - 1)]
    remote(arrived, arrived, send_sem.at[8], recv_sem.at[8], in_peer(1)).wait()

    lane8 = lax.broadcasted_iota(jnp.int32, (8, PX), 1)
    row8 = lax.broadcasted_iota(jnp.int32, (8, PX), 0)
    everyone = [ex[pl.ds(k * N_IN, N_IN), :] for k in range(NZL)]
    total = None
    for k in reversed(range(NZL)):
        part = jnp.sum(everyone[k], axis=0, keepdims=True)
        total = jnp.broadcast_to(part, (8, PX)) if total is None else jnp.where(row8 == k, part, total)
    gram = {}
    for n, (i, j) in enumerate(PAIRS):
        value = jnp.sum(jnp.where(lane8 == 64 + n, total, 0.0), axis=1, keepdims=True)
        gram[i, j] = gram[j, i] = value

    def form(p, q, offset):
        value = None
        for i, a in enumerate(p):
            for j, b in enumerate(q):
                term = a * b * gram[i, j + offset]
                value = term if value is None else value + term
        return value

    res = [jnp.ones((8, 1), jnp.float32)]
    direction, previous = list(res), []
    rr = form(res, res, 0)
    dd, beta = rr, None
    answer = [jnp.zeros((8, 1), jnp.float32) for _ in range(ITERS)]
    for step in range(ITERS):
        delta = width * form(direction, direction, 1)
        if step:
            delta = delta + sigma * (beta * beta * dd_before)
        inverse = 1.0 / (sigma * rr + delta)
        alpha = rr * inverse
        for j, value in enumerate(direction):
            answer[j] = answer[j] + alpha * value
        moved = []
        for j in range(step + 2):
            value = None
            if j <= step:
                value = res[j] * delta
                if j < len(previous):
                    value = value - sigma * rr * (beta * previous[j])
                value = value * inverse
            if j:
                part = (alpha * width) * direction[j - 1]
                value = -part if value is None else value - part
            moved.append(value)
        if step + 1 < ITERS:
            new = form(moved, moved, 0)
            beta = new / rr
            previous = direction
            direction = [
                value + beta * direction[j] if j <= step else value for j, value in enumerate(moved)
            ]
            dd_before = dd
            dd = new + beta * beta * dd
            rr = new
        res = moved

    factors = jnp.zeros((8, PX), jnp.float32)
    for k in range(ITERS + 1):
        factors = jnp.where(lane8 // 16 == k, res[k], factors)
    units = jnp.zeros((8, PX), jnp.float32)
    for k in range(NZL):
        mixed = everyone[k] * factors[k : k + 1, :]
        mixed = (mixed + pltpu.roll(mixed, PX - 16, 1)) + (
            pltpu.roll(mixed, PX - 32, 1) + pltpu.roll(mixed, PX - 48, 1)
        )
        mixed = jnp.where(lane8 < 8, mixed, 0.0) + pltpu.roll(
            jnp.where((lane8 >= 8) & (lane8 < 16), mixed, 0.0), 56, 1
        )
        mixed = pltpu.roll(mixed, 0, 1, stride=KC, stride_axis=0)
        units = jnp.where(row8 == k, jnp.sum(mixed, axis=0, keepdims=True), units)
    spot_row = pl.multiple_of(y * 16 + core * 8, 8)
    ag[pl.ds(spot_row, 8), :] = units
    mine = ag.at[pl.ds(spot_row, 8)]
    for k in range(NY):
        for o in (0, 1):
            if k or o:
                remote(mine, mine, send_sem.at[9], recv_sem.at[9], y_peer(k, o)).start()

    def own_of(value):
        value = jnp.sum(jnp.where(row8 == zl, value, 0.0), axis=0, keepdims=True)
        return value

    wide = [own_of(value) for value in res]
    wide_x = [own_of(value) for value in answer]

    def face_of(layer, faces):
        for c in range(COMP):
            a0, a1, a2, a3 = v0[c, layer + H], v1[c, layer + H], v2[c, layer + H], v3[c, layer]
            left = (wide[0] * a0 + wide[1] * a1) + (wide[2] * a2 + wide[3] * a3)
            place = c * CZ + layer
            faces = jnp.where(lane == place, pltpu.roll(left, place + 1, 1), faces)
            faces = jnp.where(lane == place + 32, pltpu.roll(left, place + 32, 1), faces)
        return faces

    faces = lax.fori_loop(0, CZ, face_of, jnp.zeros((PY, PX), jnp.float32))
    faces = jnp.transpose(jnp.concatenate([faces, jnp.zeros((PX - PY, PX), jnp.float32)], axis=0))
    left_out[...] = faces[32:64, :]
    left_copy = remote(left_out, left_in, send_sem.at[10], recv_sem.at[10], sub_prev)
    left_copy.start()

    def solve_of(layer):
        for c in range(COMP):
            a0, a1, a2 = v0[c, layer + H], v1[c, layer + H], v2[c, layer + H]
            sol_out[c, layer] = wide_x[0] * a0 + wide_x[1] * a1 + wide_x[2] * a2

    layers(0, CZ, solve_of)
    load_inv.wait()
    left_copy.wait()
    summed = faces[0:32, :] + left_in[...]
    pl.when(has_up)(send_b_up.wait_send)
    pl.when(has_down)(send_b_down.wait_send)
    pl.when(has_down)(send_m_down.wait_send)
    pl.when(has_up)(send_w1_up.wait_send)
    pl.when(has_down)(send_w1_down.wait_send)
    pl.when(has_down)(send_w2_down.wait_send)
    pl.when(has_up)(send_pack_up.wait_send)
    pl.when(inn == up_via)(pass_up.wait_send)
    pl.when(inn == down_via)(pass_down.wait_send)
    arrived = ag.at[pl.ds(0, 8 * (2 * NY - 1))]
    remote(arrived, arrived, send_sem.at[9], recv_sem.at[9], in_peer(1)).wait()

    even = [ag[pl.ds(k, NY, stride=16), :] for k in range(NZL)]
    odd = [ag[pl.ds(8 + k, NY, stride=16), :] for k in range(NZL)]
    turned_even = [pltpu.roll(value, NY - 1, 0) for value in even]
    acc = jnp.zeros((KC, PX), jnp.float32)
    for k in range(NZL):
        after = jnp.where(row8 == NY - 1, turned_even[(k + 1) % NZL], turned_even[k])
        block = jnp.where(lane8 < 64, even[k], after) + pltpu.roll(odd[k], 64, 1)
        for at in range(NY):
            column = (k * NY + at) * PX
            acc = acc + cinv[:, column : column + PX] * block[at : at + 1, :]
    coarse = jnp.sum(acc, axis=1, keepdims=True)
    spots = row * PY + lane
    for j in range(KC):
        hit = (spots == ci_own[0, j]) & (lane < PY)
        summed = summed + jnp.where(hit, coarse[j : j + 1, :], 0.0)
    for c in range(COMP):
        face_out[0, c] = summed[c * CZ : (c + 1) * CZ, 0:PY]


def on_device(body_load, materials, material_tables, corner_index, coarse_inverse):
    f32, i32 = jnp.float32, jnp.int32
    anywhere = pl.BlockSpec(memory_space=pl.ANY)
    vmem = pl.BlockSpec(memory_space=pltpu.VMEM)
    layer = (COMP, PY, PX)
    return pl.pallas_call(
        kernel,
        out_shape=(
            pltpu.VMEM((COMP, CZ, PY, PX), f32),
            pltpu.VMEM((1, COMP, CZ, PY), f32),
        ),
        in_specs=[anywhere] * 5,
        out_specs=(vmem, vmem),
        scratch_shapes=[
            pltpu.VMEM((COMP, EXT, PY, PX), f32),
            pltpu.VMEM((COMP, EXT, PY, PX), f32),
            pltpu.VMEM((COMP, EXT, PY, PX), f32),
            pltpu.VMEM((COMP, CZ, PY, PX), f32),
            pltpu.VMEM(layer, f32),
            pltpu.VMEM((EXT, PY, PX), i32),
            pltpu.VMEM((COMP * COMP, EXT, PY, PX), f32),
            pltpu.VMEM(layer, f32),
            pltpu.VMEM(layer, f32),
            pltpu.VMEM(layer, f32),
            pltpu.VMEM(layer, f32),
            pltpu.VMEM((16, PX), f32),
            pltpu.VMEM((16, PX), f32),
            pltpu.VMEM((KC, N_SUB * N_IN * KC), f32),
            pltpu.VMEM((PX, PX), f32),
            pltpu.VMEM((1, PX), f32),
            pltpu.VMEM((NZL * N_IN, PX), f32),
            pltpu.VMEM((NY * 16, PX), f32),
            pltpu.VMEM((PY, PX), f32),
            pltpu.VMEM((PY, PX), f32),
            pltpu.VMEM((1, KC), i32),
            pltpu.VMEM((1, KC), i32),
            pltpu.SMEM((1, KC), i32),
            pltpu.SMEM((1, KC), i32),
            pltpu.SMEM((COMP, COMP, NMAT), f32),
            pltpu.SemaphoreType.DMA((7,)),
            pltpu.SemaphoreType.DMA((12,)),
            pltpu.SemaphoreType.DMA((12,)),
        ],
        compiler_params=pltpu.CompilerParams(collective_id=0, has_side_effects=True),
    )(
        body_load,
        materials,
        jnp.transpose(material_tables, (1, 2, 0)),
        corner_index.reshape(1, KC),
        coarse_inverse,
    )


def solution(mesh):
    return jax.shard_map(
        on_device,
        mesh=mesh,
        in_specs=(
            P(None, "in", None, "sub"),
            P("in", None, "sub"),
            P(),
            P(("sub", "in")),
            P(("sub", "in"), None),
        ),
        out_specs=(P(None, "in", None, "sub"), P("sub", None, "in", None)),
        check_vma=False,
    )
```

```python
import jax
import jax.numpy as jnp
from jax import lax
from jax.experimental import pallas as pl
from jax.experimental.pallas import tpu as pltpu
from jax.sharding import PartitionSpec as P

MESH = pl.DeviceIdType.MESH
COMP, NMAT, ITERS = 4, 8, 3
CZ, PY, PX, KC = 8, 32, 128, 8
N_SUB, N_IN = 96, 8
H = 1
EXT = CZ + 2 * H
FIRST, LAST, BELOW, ABOVE = H, H + CZ - 1, 0, H + CZ
NX_CHIPS, NY, NZL = 4, 8, 6
FARTHEST = [(dx, dz) for dz in range(2 * NZL) for dx in range(NX_CHIPS) if dx or dz]
FARTHEST.sort(key=lambda d: -(min(d[0], NX_CHIPS - d[0]) + min(d[1], 2 * NZL - d[1])))
PAIRS = [(0, 0), (0, 1), (0, 2), (0, 3), (1, 1), (1, 2), (1, 3), (2, 2), (2, 3)]


def remote(src, dst, send, recv, device):
    return pltpu.make_async_remote_copy(
        src_ref=src, dst_ref=dst, send_sem=send, recv_sem=recv, device_id=device, device_id_type=MESH
    )


def kernel(
    b_hbm, m_hbm, tab_hbm, ci_hbm, cinv_hbm,
    sol_out, face_out,
    v0, v1, v2, v3, relay, mat, gains, w1_low, w1_high, w2_low, w2_in, pack_out, pack_in,
    cinv, rows, send_row, ex, ag, left_out, left_in,
    ci_vec, ci_left_vec, ci_own, ci_left, tab, local_sem, send_sem, recv_sem,
):
    sub, inn = lax.axis_index("sub"), lax.axis_index("in")
    core, y, zl = sub % 2, (sub // 2) % NY, sub // (2 * NY)
    x, z = inn // 2, (inn % 2) * NZL + zl

    def in_peer(k):
        return {"sub": sub, "in": (inn + k) % N_IN}

    def plane_peer(dx, dz):
        z_ = (z + dz) % (2 * NZL)
        return {"sub": ((z_ % NZL) * NY + y) * 2 + core, "in": ((x + dx) % NX_CHIPS) * 2 + z_ // NZL}

    def y_peer(k, other):
        return {"sub": (zl * NY + (y + k) % NY) * 2 + (core + other) % 2, "in": inn}

    sub_next = {"sub": (sub + 1) % N_SUB, "in": inn}
    sub_prev = {"sub": (sub + N_SUB - 1) % N_SUB, "in": inn}

    barrier = pltpu.get_barrier_semaphore()
    greet = [in_peer(1), in_peer(N_IN - 1)]
    greet += [plane_peer(dx, dz) for dz in range(2 * NZL) for dx in range(NX_CHIPS) if dx or dz]
    greet += [y_peer(k, o) for k in range(NY) for o in (0, 1) if k or o]
    greet += [sub_next, sub_prev]
    for peer in greet:
        pl.semaphore_signal(barrier, inc=1, device_id=peer, device_id_type=MESH)

    load_b = pltpu.make_async_copy(b_hbm, v0.at[:, pl.ds(H, CZ)], local_sem.at[0])
    load_m = pltpu.make_async_copy(m_hbm, mat.at[pl.ds(H, CZ)], local_sem.at[1])
    load_t = pltpu.make_async_copy(tab_hbm, tab, local_sem.at[6])
    load_c = pltpu.make_async_copy(ci_hbm, ci_vec, local_sem.at[2])
    load_inv = pltpu.make_async_copy(cinv_hbm, cinv, local_sem.at[3])
    load_own = pltpu.make_async_copy(ci_hbm, ci_own, local_sem.at[4])
    for load in (load_b, load_m, load_t, load_c, load_own, load_inv):
        load.start()
    load_t.wait()

    low, high = None, None
    for k in range(NMAT):
        for c in range(COMP):
            centre = tab[c, c, k]
            radius = jnp.float32(6.0)
            for d in range(COMP):
                if d != c:
                    radius = radius + jnp.maximum(tab[c, d, k], -tab[c, d, k])
            lo, hi = centre - radius, centre + radius
            low = lo if low is None else jnp.minimum(low, lo)
            high = hi if high is None else jnp.maximum(high, hi)
    sigma = 6.0 + 0.5 * (low + high)
    width = 0.5 * (high - low)
    inv_row = 1.0 / jnp.full((1, PX), width, jnp.float32)
    shift = 6.0 - sigma
    keep_low = jnp.where(inn > 0, jnp.float32(1.0), jnp.float32(0.0))
    keep_high = jnp.where(inn < N_IN - 1, jnp.float32(1.0), jnp.float32(0.0))
    cross = -inv_row
    cross_low, cross_high = cross * keep_low, cross * keep_high

    load_b.wait()
    load_m.wait()
    load_c.wait()
    load_own.wait()
    pl.semaphore_wait(barrier, len(greet))

    up, down = in_peer(1), in_peer(N_IN - 1)
    send_b_up = remote(v0.at[:, LAST], v0.at[:, BELOW], send_sem.at[0], recv_sem.at[0], up)
    send_b_down = remote(v0.at[:, FIRST], v0.at[:, ABOVE], send_sem.at[1], recv_sem.at[1], down)
    send_m_down = remote(mat.at[FIRST], mat.at[ABOVE], send_sem.at[2], recv_sem.at[2], down)
    send_w1_up = remote(w1_high, v1.at[:, BELOW], send_sem.at[3], recv_sem.at[3], up)
    send_w1_down = remote(w1_low, v1.at[:, ABOVE], send_sem.at[4], recv_sem.at[4], down)
    send_w2_down = remote(w2_low, w2_in, send_sem.at[5], recv_sem.at[5], down)
    send_pack_up = remote(pack_out, pack_in, send_sem.at[6], recv_sem.at[6], up)
    send_ci = remote(ci_vec, ci_left_vec, send_sem.at[7], recv_sem.at[7], sub_next)
    up_relayed, up_via, down_relayed, down_via = N_IN - 3, N_IN - 1, 2, 0
    has_up, has_down = inn < N_IN - 1, inn > 0

    def to(index):
        return {"sub": sub, "in": index}

    relay_up = remote(v0.at[:, LAST], relay, send_sem.at[0], recv_sem.at[11], to(up_via))
    relay_down = remote(v0.at[:, FIRST], relay, send_sem.at[1], recv_sem.at[11], to(down_via))
    pass_up = remote(relay, v0.at[:, BELOW], send_sem.at[11], recv_sem.at[0], to(up_relayed + 1))
    pass_down = remote(relay, v0.at[:, ABOVE], send_sem.at[11], recv_sem.at[1], to(down_relayed - 1))
    pl.when(inn == down_relayed)(relay_down.start)
    pl.when(inn == up_relayed)(relay_up.start)
    pl.when(has_down & (inn != down_relayed))(send_b_down.start)
    pl.when(has_up & (inn != up_relayed))(send_b_up.start)
    pl.when(has_down)(send_m_down.start)
    send_ci.start()

    @pl.when(inn == 0)
    def _():
        for c in range(COMP):
            v0[c, BELOW] = jnp.zeros((PY, PX), jnp.float32)
            v1[c, BELOW] = jnp.zeros((PY, PX), jnp.float32)
        pack_in[...] = jnp.zeros((16, PX), jnp.float32)

    @pl.when(inn == N_IN - 1)
    def _():
        mat[ABOVE] = jnp.zeros((PY, PX), jnp.int32)
        for c in range(COMP):
            v0[c, ABOVE] = jnp.zeros((PY, PX), jnp.float32)
            v1[c, ABOVE] = jnp.zeros((PY, PX), jnp.float32)
            w2_in[c] = jnp.zeros((PY, PX), jnp.float32)

    lane = lax.broadcasted_iota(jnp.int32, (PY, PX), 1)
    row = lax.broadcasted_iota(jnp.int32, (PY, PX), 0)

    def tables_of(layer, ids=None):
        ids = mat[layer] if ids is None else ids
        top, mid, bottom = ids >= 4, (ids & 2) != 0, (ids & 1) != 0
        for c in range(COMP):
            for d in range(COMP):
                pairs = [jnp.where(bottom, tab[c, d, 2 * k + 1], tab[c, d, 2 * k]) for k in range(4)]
                value = jnp.where(top, jnp.where(mid, pairs[3], pairs[2]), jnp.where(mid, pairs[1], pairs[0]))
                gains[c * COMP + d, layer] = value + shift if c == d else value

    def within(centre, layer):
        result = []
        for c in range(COMP):
            v = centre[c]
            beside = jnp.where(row == 0, 0.0, pltpu.roll(v, 1, 0))
            beside = beside + jnp.where(row == PY - 1, 0.0, pltpu.roll(v, PY - 1, 0))
            beside = beside + jnp.where(lane == 0, 0.0, pltpu.roll(v, 1, 1))
            beside = beside + jnp.where(lane == PX - 1, 0.0, pltpu.roll(v, PX - 1, 1))
            coupled = gains[c * COMP, layer] * centre[0]
            for d in range(1, COMP):
                coupled = coupled + gains[c * COMP + d, layer] * centre[d]
            result.append(coupled - beside)
        return result

    def take(src, layer):
        return [src[c, layer] for c in range(COMP)]

    def put(dst, layer, values):
        for c in range(COMP):
            dst[c, layer] = values[c]

    def apply_at(src, layer, below=True, above=True):
        centre = take(src, layer)
        result = within(centre, layer)
        for c in range(COMP):
            if below:
                result[c] = result[c] - src[c, layer - 1]
            if above:
                result[c] = result[c] - src[c, layer + 1]
        return centre, [value * inv_row for value in result]

    def layers(lo, hi, body):
        @pl.loop(lo, hi)
        def _(layer):
            body(layer)

    def products(sums, basis, only=None):
        out = []
        for (i, j), total in zip(PAIRS, sums):
            if basis[j] is None or only not in (None, j):
                out.append(total)
                continue
            part = basis[i][0] * basis[j][0]
            for c in range(1, COMP):
                part = part + basis[i][c] * basis[j][c]
            out.append(total + ((part[0:8] + part[8:16]) + (part[16:24] + part[24:32])))
        return tuple(out)

    def third(layer, sums, below=True):
        a2, a3 = apply_at(v2, layer, below=below)
        put(v3, layer - H, a3)
        return products(sums, (take(v0, layer), take(v1, layer), a2, a3))

    def across(sums):
        mine = [cross_high * value for value in take(v2, LAST)]
        out = list(sums)
        for i, source in enumerate((v0, v1, v2)):
            part = source[0, ABOVE] * mine[0]
            for c in range(1, COMP):
                part = part + source[c, ABOVE] * mine[c]
            n = PAIRS.index((i, 3))
            out[n] = out[n] + ((part[0:8] + part[8:16]) + (part[16:24] + part[24:32]))
        return tuple(out)

    def first(layer):
        put(v1, layer, apply_at(v0, layer)[1])

    def second(layer):
        put(v2, layer, apply_at(v1, layer)[1])

    layers(FIRST, FIRST + 2, tables_of)
    layers(LAST - 1, LAST + 1, tables_of)
    low1 = apply_at(v0, FIRST, below=False)[1]
    put(v1, FIRST, low1)
    high1 = apply_at(v0, LAST, above=False)[1]
    put(v1, LAST, high1)
    for c in range(COMP):
        w1_low[c] = low1[c]
        w1_high[c] = high1[c]
    pl.when(has_down)(send_w1_down.start)
    pl.when(has_up)(send_w1_up.start)
    first(FIRST + 1)
    first(LAST - 1)
    low2 = apply_at(v1, FIRST, below=False)[1]
    for c in range(COMP):
        w2_low[c] = low2[c]
    pl.when(has_down)(send_w2_down.start)
    high2 = apply_at(v1, LAST, above=False)[1]
    packed = jnp.zeros((PY, PX), jnp.float32)
    for c, value in enumerate(high2 + [mat[LAST].astype(jnp.float32)]):
        packed = jnp.where(lane == c, pltpu.roll(value, c + 1, 1), packed)
        packed = jnp.where(lane == 8 + c, pltpu.roll(value, 8 + c, 1), packed)
    blank = jnp.zeros((PX - PY, PX), jnp.float32)
    pack_out[...] = jnp.transpose(jnp.concatenate([packed, blank], axis=0))[0:16, :]
    pl.when(has_up)(send_pack_up.start)

    layers(FIRST + 2, LAST - 1, tables_of)
    layers(FIRST + 2, LAST - 1, first)
    layers(FIRST + 2, LAST - 1, second)
    sums = tuple(jnp.zeros((8, PX), jnp.float32) for _ in PAIRS)
    sums = lax.fori_loop(FIRST + 3, LAST - 2, third, sums)

    @pl.when(inn == up_via)
    def _():
        relay_up.wait_recv()
        pass_up.start()

    @pl.when(inn == down_via)
    def _():
        relay_down.wait_recv()
        pass_down.start()

    pl.when(has_up)(send_b_down.wait_recv)
    pl.when(has_up)(send_m_down.wait_recv)
    pl.when(has_down)(send_b_up.wait_recv)
    send_ci.wait()
    load_left = pltpu.make_async_copy(ci_left_vec, ci_left, local_sem.at[5])
    load_left.start()
    for c in range(COMP):
        v1[c, FIRST] = v1[c, FIRST] + cross_low * v0[c, BELOW]
        v1[c, LAST] = v1[c, LAST] + cross_high * v0[c, ABOVE]
    tables_of(ABOVE)
    second(FIRST + 1)
    second(LAST - 1)
    pl.when(has_up)(send_w1_down.wait_recv)
    pl.when(has_down)(send_w1_up.wait_recv)
    for c in range(COMP):
        v1[c, BELOW] = keep_low * v1[c, BELOW] + cross_low * v0[c, FIRST]
        v1[c, ABOVE] = keep_high * v1[c, ABOVE] + cross_high * v0[c, LAST]
    second(FIRST)
    second(LAST)
    sums = lax.fori_loop(FIRST + 1, FIRST + 3, third, sums)
    sums = lax.fori_loop(LAST - 2, LAST, third, sums)
    above = within(take(v0, LAST), ABOVE)
    above = [term * inv_row + v1[c, LAST] for c, term in enumerate(above)]
    sums = third(FIRST, sums, below=False)
    load_left.wait()
    pl.when(has_down)(send_pack_up.wait_recv)
    packed = jnp.concatenate([pack_in[...], jnp.zeros((PX - 16, PX), jnp.float32)], axis=0)
    packed = jnp.transpose(packed)[0:PY, :]

    def column(c):
        return jnp.where(lane == PX - 1, pltpu.roll(packed, PX - 1 - c, 1), pltpu.roll(packed, PX - 8 - c, 1))

    at_ends = (lane == 0) | (lane == PX - 1)
    tables_of(BELOW, jnp.where(at_ends, column(COMP), 0.0).astype(jnp.int32))
    below = within(take(v0, FIRST), BELOW)
    for c in range(COMP):
        value = keep_low * column(c) + cross_low * (below[c] * inv_row + v1[c, FIRST])
        v3[c, 0] = v3[c, 0] + cross_low * jnp.where(at_ends, value, 0.0)

    places = []
    for j in range(KC):
        for side, ids in ((0, ci_own), (1, ci_left)):
            spot = ids[0, j]
            c, layer, at = spot // (CZ * PY), (spot // PY) % CZ, spot % PY
            place = side * KC + j
            places.append((place, c, layer, at))
            rows[pl.ds(place, 1), :] = v0[c, layer + H, pl.ds(at, 1), :]
            rows[pl.ds(16 + place, 1), :] = v1[c, layer + H, pl.ds(at, 1), :]
            rows[pl.ds(32 + place, 1), :] = v2[c, layer + H, pl.ds(at, 1), :]
    rows[pl.ds(64, 64), :] = jnp.zeros((64, PX), jnp.float32)
    lane1 = lax.broadcasted_iota(jnp.int32, (1, PX), 1)

    def with_sums(into, chosen):
        for n, (i, j) in enumerate(PAIRS):
            if chosen(j):
                whole = jnp.sum(jnp.sum(sums[n], axis=0, keepdims=True), axis=1, keepdims=True)
                into = jnp.where(lane1 == 64 + n, whole, into)
        return into

    a2 = take(v2, LAST)
    a0, a1 = take(v0, LAST), take(v1, LAST)
    sums = products(sums, (a0, a1, a2, None))
    sums_row = with_sums(jnp.zeros((1, PX), jnp.float32), lambda j: j < 3)
    pl.when(has_up)(send_w2_down.wait_recv)
    for c in range(COMP):
        v2[c, ABOVE] = keep_high * w2_in[c] + cross_high * above[c]
    a3 = apply_at(v2, LAST)[1]
    put(v3, LAST - H, a3)
    sums = products(sums, (a0, a1, a2, a3), only=3)
    sums = across(sums)
    for place, c, layer, at in places:
        rows[pl.ds(48 + place, 1), :] = v3[c, layer, pl.ds(at, 1), :]
    turned = jnp.transpose(rows[...])
    own_row = jnp.where((lane1 // KC) % 2 == 0, turned[PX - 1 : PX, :], turned[0:1, :])
    own_row = jnp.where(lane1 < 64, own_row, with_sums(sums_row, lambda j: j == 3))
    send_row[...] = own_row
    ex[pl.ds(zl * N_IN + inn, 1), :] = own_row
    n_plane = 2 * NZL * NX_CHIPS
    spot = ex.at[pl.ds(zl * N_IN + inn, 1)]
    for dx, dz in FARTHEST:
        remote(send_row, spot, send_sem.at[8], recv_sem.at[8], plane_peer(dx, dz)).start()
    arrived = ex.at[pl.ds(0, n_plane - 1)]
    remote(arrived, arrived, send_sem.at[8], recv_sem.at[8], in_peer(1)).wait()

    lane8 = lax.broadcasted_iota(jnp.int32, (8, PX), 1)
    row8 = lax.broadcasted_iota(jnp.int32, (8, PX), 0)
    everyone = [ex[pl.ds(k * N_IN, N_IN), :] for k in range(NZL)]
    total = None
    for k in reversed(range(NZL)):
        part = jnp.sum(everyone[k], axis=0, keepdims=True)
        total = jnp.broadcast_to(part, (8, PX)) if total is None else jnp.where(row8 == k, part, total)
    gram = {}
    for n, (i, j) in enumerate(PAIRS):
        value = jnp.sum(jnp.where(lane8 == 64 + n, total, 0.0), axis=1, keepdims=True)
        gram[i, j] = gram[j, i] = value

    def form(p, q, offset):
        value = None
        for i, a in enumerate(p):
            for j, b in enumerate(q):
                term = a * b * gram[i, j + offset]
                value = term if value is None else value + term
        return value

    res = [jnp.ones((8, 1), jnp.float32)]
    direction, previous = list(res), []
    rr = form(res, res, 0)
    dd, beta = rr, None
    answer = [jnp.zeros((8, 1), jnp.float32) for _ in range(ITERS)]
    for step in range(ITERS):
        delta = width * form(direction, direction, 1)
        if step:
            delta = delta + sigma * (beta * beta * dd_before)
        inverse = 1.0 / (sigma * rr + delta)
        alpha = rr * inverse
        for j, value in enumerate(direction):
            answer[j] = answer[j] + alpha * value
        moved = []
        for j in range(step + 2):
            value = None
            if j <= step:
                value = res[j] * delta
                if j < len(previous):
                    value = value - sigma * rr * (beta * previous[j])
                value = value * inverse
            if j:
                part = (alpha * width) * direction[j - 1]
                value = -part if value is None else value - part
            moved.append(value)
        if step + 1 < ITERS:
            new = form(moved, moved, 0)
            beta = new / rr
            previous = direction
            direction = [
                value + beta * direction[j] if j <= step else value for j, value in enumerate(moved)
            ]
            dd_before = dd
            dd = new + beta * beta * dd
            rr = new
        res = moved

    factors = jnp.zeros((8, PX), jnp.float32)
    for k in range(ITERS + 1):
        factors = jnp.where(lane8 // 16 == k, res[k], factors)
    units = jnp.zeros((8, PX), jnp.float32)
    for k in range(NZL):
        mixed = everyone[k] * factors[k : k + 1, :]
        mixed = (mixed + pltpu.roll(mixed, PX - 16, 1)) + (
            pltpu.roll(mixed, PX - 32, 1) + pltpu.roll(mixed, PX - 48, 1)
        )
        mixed = jnp.where(lane8 < 8, mixed, 0.0) + pltpu.roll(
            jnp.where((lane8 >= 8) & (lane8 < 16), mixed, 0.0), 56, 1
        )
        mixed = pltpu.roll(mixed, 0, 1, stride=KC, stride_axis=0)
        units = jnp.where(row8 == k, jnp.sum(mixed, axis=0, keepdims=True), units)
    spot_row = pl.multiple_of(y * 16 + core * 8, 8)
    ag[pl.ds(spot_row, 8), :] = units
    mine = ag.at[pl.ds(spot_row, 8)]
    for k in sorted(range(NY), key=lambda k: -min(k, NY - k)):
        for o in (0, 1):
            if k or o:
                remote(mine, mine, send_sem.at[9], recv_sem.at[9], y_peer(k, o)).start()

    def own_of(value):
        value = jnp.sum(jnp.where(row8 == zl, value, 0.0), axis=0, keepdims=True)
        return value

    wide = [own_of(value) for value in res]
    wide_x = [own_of(value) for value in answer]

    def face_of(layer, faces):
        for c in range(COMP):
            a0, a1, a2, a3 = v0[c, layer + H], v1[c, layer + H], v2[c, layer + H], v3[c, layer]
            left = (wide[0] * a0 + wide[1] * a1) + (wide[2] * a2 + wide[3] * a3)
            place = c * CZ + layer
            faces = jnp.where(lane == place, pltpu.roll(left, place + 1, 1), faces)
            faces = jnp.where(lane == place + 32, pltpu.roll(left, place + 32, 1), faces)
        return faces

    faces = lax.fori_loop(0, CZ, face_of, jnp.zeros((PY, PX), jnp.float32))
    faces = jnp.transpose(jnp.concatenate([faces, jnp.zeros((PX - PY, PX), jnp.float32)], axis=0))
    left_out[...] = faces[32:64, :]
    left_copy = remote(left_out, left_in, send_sem.at[10], recv_sem.at[10], sub_prev)
    left_copy.start()

    def solve_of(layer):
        for c in range(COMP):
            a0, a1, a2 = v0[c, layer + H], v1[c, layer + H], v2[c, layer + H]
            sol_out[c, layer] = wide_x[0] * a0 + wide_x[1] * a1 + wide_x[2] * a2

    layers(0, CZ, solve_of)
    load_inv.wait()
    left_copy.wait()
    summed = faces[0:32, :] + left_in[...]
    pl.when(has_up)(send_b_up.wait_send)
    pl.when(has_down)(send_b_down.wait_send)
    pl.when(has_down)(send_m_down.wait_send)
    pl.when(has_up)(send_w1_up.wait_send)
    pl.when(has_down)(send_w1_down.wait_send)
    pl.when(has_down)(send_w2_down.wait_send)
    pl.when(has_up)(send_pack_up.wait_send)
    pl.when(inn == up_via)(pass_up.wait_send)
    pl.when(inn == down_via)(pass_down.wait_send)
    arrived = ag.at[pl.ds(0, 8 * (2 * NY - 1))]
    remote(arrived, arrived, send_sem.at[9], recv_sem.at[9], in_peer(1)).wait()

    even = [ag[pl.ds(k, NY, stride=16), :] for k in range(NZL)]
    odd = [ag[pl.ds(8 + k, NY, stride=16), :] for k in range(NZL)]
    turned_even = [pltpu.roll(value, NY - 1, 0) for value in even]
    acc = jnp.zeros((KC, PX), jnp.float32)
    for k in range(NZL):
        after = jnp.where(row8 == NY - 1, turned_even[(k + 1) % NZL], turned_even[k])
        block = jnp.where(lane8 < 64, even[k], after) + pltpu.roll(odd[k], 64, 1)
        for at in range(NY):
            column = (k * NY + at) * PX
            acc = acc + cinv[:, column : column + PX] * block[at : at + 1, :]
    coarse = jnp.sum(acc, axis=1, keepdims=True)
    spots = row * PY + lane
    for j in range(KC):
        hit = (spots == ci_own[0, j]) & (lane < PY)
        summed = summed + jnp.where(hit, coarse[j : j + 1, :], 0.0)
    for c in range(COMP):
        face_out[0, c] = summed[c * CZ : (c + 1) * CZ, 0:PY]


def on_device(body_load, materials, material_tables, corner_index, coarse_inverse):
    f32, i32 = jnp.float32, jnp.int32
    anywhere = pl.BlockSpec(memory_space=pl.ANY)
    vmem = pl.BlockSpec(memory_space=pltpu.VMEM)
    layer = (COMP, PY, PX)
    return pl.pallas_call(
        kernel,
        out_shape=(
            pltpu.VMEM((COMP, CZ, PY, PX), f32),
            pltpu.VMEM((1, COMP, CZ, PY), f32),
        ),
        in_specs=[anywhere] * 5,
        out_specs=(vmem, vmem),
        scratch_shapes=[
            pltpu.VMEM((COMP, EXT, PY, PX), f32),
            pltpu.VMEM((COMP, EXT, PY, PX), f32),
            pltpu.VMEM((COMP, EXT, PY, PX), f32),
            pltpu.VMEM((COMP, CZ, PY, PX), f32),
            pltpu.VMEM(layer, f32),
            pltpu.VMEM((EXT, PY, PX), i32),
            pltpu.VMEM((COMP * COMP, EXT, PY, PX), f32),
            pltpu.VMEM(layer, f32),
            pltpu.VMEM(layer, f32),
            pltpu.VMEM(layer, f32),
            pltpu.VMEM(layer, f32),
            pltpu.VMEM((16, PX), f32),
            pltpu.VMEM((16, PX), f32),
            pltpu.VMEM((KC, N_SUB * N_IN * KC), f32),
            pltpu.VMEM((PX, PX), f32),
            pltpu.VMEM((1, PX), f32),
            pltpu.VMEM((NZL * N_IN, PX), f32),
            pltpu.VMEM((NY * 16, PX), f32),
            pltpu.VMEM((PY, PX), f32),
            pltpu.VMEM((PY, PX), f32),
            pltpu.VMEM((1, KC), i32),
            pltpu.VMEM((1, KC), i32),
            pltpu.SMEM((1, KC), i32),
            pltpu.SMEM((1, KC), i32),
            pltpu.SMEM((COMP, COMP, NMAT), f32),
            pltpu.SemaphoreType.DMA((7,)),
            pltpu.SemaphoreType.DMA((12,)),
            pltpu.SemaphoreType.DMA((12,)),
        ],
        compiler_params=pltpu.CompilerParams(collective_id=0, has_side_effects=True),
    )(
        body_load,
        materials,
        jnp.transpose(material_tables, (1, 2, 0)),
        corner_index.reshape(1, KC),
        coarse_inverse,
    )


def solution(mesh):
    return jax.shard_map(
        on_device,
        mesh=mesh,
        in_specs=(
            P(None, "in", None, "sub"),
            P("in", None, "sub"),
            P(),
            P(("sub", "in")),
            P(("sub", "in"), None),
        ),
        out_specs=(P(None, "in", None, "sub"), P("sub", None, "in", None)),
        check_vma=False,
    )
```
